512 devices in a mesh: real: 2 (over y), env: 32 (over z), mpo: 4 (over x), col: 2 (over core).
Axes of the slice: x: 4, y: 2, z: 32, core: 2. Of those that a mesh axis runs over, the one named last changes fastest.
The devices are a block of a 4x8x32 slice.
Arguments:
- held: bfloat16 [24576, 8, 384], P(('real', 'env', 'col')), parts along dimension 0, may hold values from -0.15625 to 0.15625
- owner_map: int32 [64, 192], P('real'), parts along dimension 0, may hold values from 0 to 12287, as said below
- kept: int32 [64], P(('real', 'env')), parts along dimension 0, may hold values from 96 to 384
- left_env: bfloat16 [16, 64, 384, 384], P('mpo', ('real', 'env')), parts along dimension 1, may hold values from -6 to 6
- mpo_tensor: float32 [14, 14, 4, 4], replicated, may hold values from -1 to 1
- mpo_mask: int32 [14, 14], replicated, may hold values 0 or 1
- fields: float32 [4], P('real'), parts along dimension 0, may hold values from -2 to 2
Outputs:
- new_env: float32 [16, 64, 384, 384], P('mpo', ('real', 'env'), None, 'col'), parts along dimension 1
The draws below stay inside these ranges and needn't reach their ends.
There are 2 independent parts, one for each index of `real`. The reference program is written for one: setup_inputs(seed, part) draws one part's arguments, and reference() takes and returns one part's arrays. A program takes and returns all parts, laid end to end along the dimension named above; an argument that names none is the same for every part. Nothing has to cross between parts.
Inputs may be any that keep to these rules, and one draw needn't show every extreme that they name: owner_map[t, j] is the slot of held that holds tile j of sector t; all entries differ. The owner of index o along env+col holds the slots o * 192 to (o + 1) * 192 - 1. Among the tiles of one sector (the sector of one env index), one owner holds at most 6, and for every sector some owner holds exactly 6.
All inputs are finite; a program needn't handle non-finite values.
Results may differ from the reference program's by a relative error of at most 0.0042.
Values may be sent and summed in bfloat16 or wider, within the bound.
A program may use at most 64 MiB of HBM per device.

```python
import jax
import jax.numpy as jnp
from jax import lax

P_SIZE = 4
K = 14
B = 384
TILE = 8
SEC_DEV = 1
S = 32
NT = 192
CAP = 6
POOL = 192
SLOTS = 12288
KSL = 4
KP = 16
N_MPO = 4


def draw_owner_map(key, part):
    owners = 2 * SEC_DEV * NT // CAP
    row_count = S // SEC_DEV
    tiles_row = SEC_DEV * NT
    heavy = jax.random.randint(jax.random.fold_in(key, 11), (owners,), 0, 4)
    order = jax.vmap(lambda sub: jax.random.permutation(sub, POOL))(jax.random.split(jax.random.fold_in(key, 12), owners))

    def one_row(row):
        row_key = jax.random.fold_in(jax.random.fold_in(key, 13), row)
        candidate = jnp.arange(owners * CAP, dtype=jnp.int32)
        cand_owner = candidate // CAP
        noise = jax.random.randint(jax.random.fold_in(row_key, 1), (owners * CAP,), 0, 4096)
        forced = jax.random.randint(jax.random.fold_in(row_key, 2), (), 0, owners)
        score = noise + heavy[cand_owner] * 2048 + jnp.where(cand_owner == forced, 32768, 0)
        score = score * (owners * CAP) + candidate
        unused, chosen = lax.top_k(score, tiles_row)
        chosen = jax.random.permutation(jax.random.fold_in(row_key, 3), chosen)
        chosen_owner = chosen // CAP
        chosen_rank = chosen % CAP
        position = order[chosen_owner, row * CAP + chosen_rank]
        return chosen_owner * POOL + position
    table = jax.vmap(one_row)(jnp.arange(row_count, dtype=jnp.int32))
    return table.reshape(S, NT).astype(jnp.int32)


def with_ends(drawn, key, least, largest):
    longest = drawn.shape.index(max(drawn.shape))
    spots = []
    for shift in (0, 1):
        where = [jax.random.randint(jax.random.fold_in(key, axis), (), 0, length) for axis, length in enumerate(drawn.shape)]
        where[longest] = (where[longest] + shift) % drawn.shape[longest]
        spots.append(tuple(where))
    return drawn.at[spots[0]].set(least).at[spots[1]].set(largest)


def block_scale(stream_key, shape, shards, smallest, top_value):
    factor_of = 1.0
    for axis_at, blocks in shards:
        steps = jax.random.uniform(jax.random.fold_in(jax.random.fold_in(stream_key, 6), axis_at), (blocks,), jnp.float32, smallest / len(shards), top_value / len(shards))
        factor_of = factor_of * jnp.repeat(jnp.exp(steps), shape[axis_at] // blocks).reshape((-1,) + (1,) * (len(shape) - 1 - axis_at))
    return factor_of


def bell_draw(own_key, dims, width, limit, pieces=(), held_as=jnp.bfloat16):
    drawn = width * jax.random.normal(own_key, dims, jnp.float32)
    if pieces:
        drawn = drawn * block_scale(own_key, dims, pieces, -0.22, 0.18)
    return jnp.clip(drawn, -limit, limit).astype(held_as)


def setup_inputs(seed: int = 0, part: int = 0) -> dict:
    splits = jax.random.split(jax.random.key(seed), 8)
    own_keys = jax.random.split(jax.random.fold_in(splits[7], part), 8)
    return {
        "held": bell_draw(own_keys[0], (SLOTS, TILE, B), (P_SIZE * B) ** -0.5, 0.15625, ((0, 64),)),
        "owner_map": draw_owner_map(jax.random.fold_in(jax.random.fold_in(splits[7], part), 71), part),
        "kept": with_ends(jax.random.randint(own_keys[2], (S,), B // 4, B + 1), jax.random.fold_in(own_keys[2], 1), B // 4, B).astype(jnp.int32),
        "left_env": bell_draw(own_keys[3], (KP, S, B, B), 1.0, 6.0, ((0, 4), (1, 32))),
        "mpo_tensor": bell_draw(splits[4], (K, K, P_SIZE, P_SIZE), (K * P_SIZE // 2) ** -0.5, 1.0, (), jnp.float32),
        "mpo_mask": with_ends((jax.random.randint(splits[5], (K, K), 0, 2) < 1).astype(jnp.int32), jax.random.fold_in(splits[5], 1), 0, 1),
        "fields": jnp.clip(jax.random.uniform(own_keys[6], (2,), jnp.float32, -2.0, 2.0), -2.0, 2.0),
    }


def build_couplings(mpo_tensor, mpo_mask, fields, padded):
    bond = mpo_tensor.shape[0]
    states = mpo_tensor.shape[2]
    base = mpo_tensor * mpo_mask.astype(jnp.float32)[:, :, None, None]
    level = jnp.arange(states, dtype=jnp.int32)
    spin_first = 0.5 - (level // 2).astype(jnp.float32)
    spin_second = 0.5 - (level % 2).astype(jnp.float32)
    onsite = jnp.diag(fields[0] * spin_first + fields[1] * spin_second)
    bond_index = jnp.arange(bond, dtype=jnp.int32)
    corner = (bond_index[:, None] == bond - 1) & (bond_index[None, :] == 0)
    base = base + jnp.where(corner[:, :, None, None], onsite[None, None, :, :], jnp.float32(0.0))
    return jnp.pad(base, ((0, padded - bond), (0, padded - bond), (0, 0), (0, 0)))


def reference(held, owner_map, kept, left_env, mpo_tensor, mpo_mask, fields):
    tiles = jnp.take(held, owner_map.reshape(-1), axis=0)
    sector_matrices = tiles.reshape(S, P_SIZE, B, B)
    columns = jnp.arange(B, dtype=jnp.int32)
    keep = columns[None, :] < kept[:, None]
    sector_matrices = jnp.where(keep[:, None, None, :], sector_matrices, jnp.zeros((), jnp.bfloat16))
    couplings = build_couplings(mpo_tensor, mpo_mask, fields, KP)
    leading_sector = lax.Precision.HIGHEST

    def one_sector(pair):
        block, environment = pair
        bond_vectors = block.astype(jnp.float32)
        first = jnp.einsum("wij,sja->wsia", environment[:K].astype(jnp.float32), bond_vectors, precision=leading_sector)
        contracted_sum = jnp.zeros((K, P_SIZE, B, B), jnp.float32)
        for slab_index in range(N_MPO):
            lower = slab_index * KSL
            upper = min(lower + KSL, K)
            if lower < K:
                next_spin = jnp.einsum("wvts,wsia->vtia", couplings[lower:upper, :K], first[lower:upper], precision=leading_sector)
                rounded = lax.optimization_barrier(next_spin.astype(jnp.bfloat16))
                contracted_sum = contracted_sum + rounded.astype(jnp.float32)
        updated_environment = jnp.einsum("hze,shzo->seo", bond_vectors, contracted_sum, precision=leading_sector)
        return jnp.pad(updated_environment, ((0, KP - K), (0, 0), (0, 0)))

    stacked = lax.map(one_sector, (sector_matrices, jnp.moveaxis(left_env, 1, 0)))
    return jnp.moveaxis(stacked, 0, 1)
```

```python
import functools

import jax
import jax.numpy as jnp
from jax import lax
from jax.experimental import pallas as pl
from jax.experimental.pallas import tpu as pltpu
from jax.sharding import PartitionSpec as P

MESH = pl.DeviceIdType.MESH
VMEM = pltpu.VMEM
SMEM = pltpu.SMEM
DMA = pltpu.SemaphoreType.DMA
LANES = 128
ROWS = 16


def plan_kernel(pool, cap, thirds, sectors, map_ref, src_ref, idx_ref):
    tiles = map_ref.shape[1]
    row = lax.axis_index("env")
    me = row * lax.axis_size("col") + lax.axis_index("col")
    slots = map_ref[...]
    local = slots - me * pool
    mine = (local >= 0) & (local < pool)
    before = lax.broadcasted_iota(jnp.int32, (tiles, tiles), 0) < lax.broadcasted_iota(jnp.int32, (tiles, tiles), 1)
    rank = jnp.dot(
        jnp.where(mine, 1.0, 0.0).astype(jnp.bfloat16),
        jnp.where(before, 1.0, 0.0).astype(jnp.bfloat16),
        preferred_element_type=jnp.float32,
    )
    lane = lax.broadcasted_iota(jnp.int32, src_ref.shape, 1)
    found = jnp.zeros(src_ref.shape, jnp.float32)
    localf = local.astype(jnp.float32)
    for r in range(cap):
        slot = jnp.sum(jnp.where(mine & (rank == float(r)), localf, 0.0), axis=1, keepdims=True)
        found = jnp.where(lane == r, slot, found)
    src_ref[...] = found.astype(jnp.int32)
    own = map_ref[pl.ds(row, 1), :].astype(jnp.float32)
    owner = jnp.floor((own + 0.5) * (1.0 / pool))
    same = lax.broadcasted_iota(jnp.int32, (tiles, tiles), 0) == lax.broadcasted_iota(jnp.int32, (tiles, tiles), 1)
    column = jnp.sum(jnp.where(same, jnp.broadcast_to(owner, (tiles, tiles)), 0.0), axis=1, keepdims=True)
    order = jnp.sum(jnp.where((column == owner) & before, 1.0, 0.0), axis=0, keepdims=True)
    idx_ref[...] = (owner * float(cap * thirds) + order * float(thirds)).astype(jnp.int32)


def main_kernel(
    dims, src_ref, idx_ref, kept_ref, held_ref, left_ref, pair_ref, out_ref,
    units, sent5, sent4, relay5, relay4, lefts, kron, mixed, block, flipped, second,
    load_sem, near5_s, near5_r, near4_s, near4_r, bund_s, bund_r, x_s, x_r, f_s, f_r, d_s, d_r, ls, lr,
):
    n, nx, cap, thirds, bond = dims
    per = cap * thirds
    slab = left_ref.shape[0]
    width = left_ref.shape[2]
    half = n // 2
    hop = n // 4
    z, x, c = lax.axis_index("env"), lax.axis_index("mpo"), lax.axis_index("col")
    states = block.shape[0] // width
    even = lax.rem(x + c, 2) == 0
    sgn = jnp.where(even, 1, -1)

    def start5(p):
        return 4 * p + p // 2

    def start4(p):
        return 5 * p - p // 2

    def at_z(off):
        return lax.rem(z + off + n, n)

    def at_x(off):
        return lax.rem(x + off + nx, nx)

    def rcopy(src, dst, ss, rs, where):
        return pltpu.make_async_remote_copy(src_ref=src, dst_ref=dst, send_sem=ss, recv_sem=rs, device_id=where, device_id_type=MESH)

    load = pltpu.make_async_copy(left_ref, lefts.at[pl.ds(x * slab, slab)], load_sem)
    load.start()

    barrier = pltpu.get_barrier_semaphore()

    def greet(k, _):
        pl.semaphore_signal(barrier, inc=1, device_id={"env": at_z(k)}, device_id_type=MESH)
        pl.semaphore_signal(barrier, inc=1, device_id={"env": at_z(-k)}, device_id_type=MESH)
        return 0

    lax.fori_loop(1, hop + 1, greet, 0)
    pl.semaphore_signal(barrier, inc=1, device_id={"mpo": at_x(1)}, device_id_type=MESH)
    pl.semaphore_signal(barrier, inc=1, device_id={"mpo": at_x(-1)}, device_id_type=MESH)
    pl.semaphore_signal(barrier, inc=1, device_id={"col": 1 - c}, device_id_type=MESH)

    def unit(t, u):
        r, h = u // thirds, lax.rem(u, thirds)
        return held_ref[src_ref[t, r], :, pl.ds(pl.multiple_of(h * LANES, LANES), LANES)]

    u5, u4 = start5(x), start4(x)

    def pick(k, _):
        t5, t4 = at_z(sgn * (k + 1)), at_z(-sgn * (k + 1))
        for i in range(5):
            sent5[k, i] = unit(t5, u5 + i)
        for i in range(4):
            sent4[k, i] = unit(t4, u4 + i)
        return 0

    lax.fori_loop(0, half, pick, 0)

    def own(u, _):
        units[(z * 2 + c) * per + u] = unit(z, u)
        return 0

    lax.fori_loop(0, per, own, 0)

    load.wait()
    pl.semaphore_wait(barrier, 2 * hop + 3)

    def slot(zz, first, count):
        return units.at[pl.ds((zz * 2 + c) * per + first, count)]

    lo = c * (width // 2)

    def rows_of(p, core_lo):
        return lefts.at[pl.ds(p * slab, slab), pl.ds(pl.multiple_of(core_lo, ROWS), width // 2)]

    lsend = []
    for k, off in enumerate((1, -1)):
        cp = rcopy(rows_of(x, lo), rows_of(x, lo), ls.at[k], lr.at[k], {"mpo": at_x(off)})
        cp.start()
        lsend.append(cp)

    far5 = rcopy(sent5.at[pl.ds(hop, hop)], relay5, bund_s.at[0], bund_r.at[0], {"env": at_z(sgn * hop)})
    far4 = rcopy(sent4.at[pl.ds(hop, hop)], relay4, bund_s.at[1], bund_r.at[1], {"env": at_z(-sgn * hop)})
    far5.start()
    far4.start()

    def near_copies(k):
        a = rcopy(sent5.at[k], slot(z, u5, 5), near5_s.at[k], near5_r.at[k], {"env": at_z(sgn * (k + 1))})
        b = rcopy(sent4.at[k], slot(z, u4, 4), near4_s.at[k], near4_r.at[k], {"env": at_z(-sgn * (k + 1))})
        return a, b

    def near(i, _):
        a, b = near_copies(hop - 1 - i)
        a.start()
        b.start()
        return 0

    lax.fori_loop(0, hop, near, 0)

    def d2d(zz, k):
        return rcopy(slot(zz, 0, per), slot(zz, 0, per), d_s.at[k], d_r.at[k], {"col": 1 - c})

    d2d(z, n - 1).start()

    rowi = lax.broadcasted_iota(jnp.int32, (kron.shape[0] // 8, pair_ref.shape[0]), 0)
    coli = lax.broadcasted_iota(jnp.int32, (kron.shape[0] // 8, pair_ref.shape[0]), 1)
    kk = kron.shape[1]
    wi = lax.broadcasted_iota(jnp.int32, (pair_ref.shape[1], kk), 0)
    wc = lax.broadcasted_iota(jnp.int32, (pair_ref.shape[1], kk), 1)
    wk = wc // ROWS + jnp.where(wc < bond * ROWS, 0, pair_ref.shape[1] // 2 - bond)
    spread = jnp.where(wk == wi, 1.0, 0.0).astype(jnp.bfloat16)
    rr = lax.broadcasted_iota(jnp.int32, (kron.shape[0] // 8, kk), 0)
    cc = lax.broadcasted_iota(jnp.int32, (kron.shape[0] // 8, kk), 1)
    diag = lax.rem(rr, ROWS) == lax.rem(cc, ROWS)
    pairs = jnp.dot(pair_ref[...], spread, preferred_element_type=jnp.float32).astype(jnp.bfloat16)

    def build(g, _):
        pickrow = (rowi // ROWS) + g * (kron.shape[0] // 8 // ROWS) == coli
        full = jnp.dot(jnp.where(pickrow, 1.0, 0.0).astype(jnp.bfloat16), pairs, preferred_element_type=jnp.float32)
        kron[pl.ds(g * (kron.shape[0] // 8), kron.shape[0] // 8), :] = jnp.where(diag, full, 0.0).astype(jnp.bfloat16)
        return 0

    lax.fori_loop(0, 8, build, 0)

    fdir = 1 - 2 * c
    pside = {"col": 1 - c}
    from_below = rcopy(rows_of(at_x(-1), lo), rows_of(at_x(-1), lo), ls.at[3], lr.at[3], pside)
    from_above = rcopy(rows_of(at_x(1), lo), rows_of(at_x(1), lo), ls.at[4], lr.at[4], pside)
    lsend[0].wait_recv()
    lsend[1].wait_recv()
    fwd = rcopy(rows_of(at_x(-fdir), lo), rows_of(at_x(-fdir), lo), ls.at[2], lr.at[2], {"mpo": at_x(fdir)})
    fwd.start()
    from_below.start()
    from_above.start()

    def relay_copies(k):
        src5 = at_z(-sgn * hop)
        return rcopy(relay5.at[k], slot(src5, u5, 5), near5_s.at[hop + k], near5_r.at[hop + k], {"env": at_z(sgn * (k + 1))})

    def relay_copies4(k):
        src4 = at_z(sgn * hop)
        return rcopy(relay4.at[k], slot(src4, u4, 4), near4_s.at[hop + k], near4_r.at[hop + k], {"env": at_z(-sgn * (k + 1))})

    far5.wait_recv()
    far4.wait_recv()

    @pl.when(even)
    def _():
        relay_copies(hop - 1).start()

    @pl.when(jnp.logical_not(even))
    def _():
        relay_copies4(hop - 1).start()

    def relay(i, _):
        relay_copies(hop - 2 - i).start()
        relay_copies4(hop - 2 - i).start()
        return 0

    lax.fori_loop(0, hop - 1, relay, 0)

    def x_send(kind, k):
        zz = at_z(-sgn * (k + 1)) if kind == 0 else at_z(sgn * (k + 1))
        ref = slot(zz, u5, 5) if kind == 0 else slot(zz, u4, 4)
        return (
            rcopy(ref, ref, x_s.at[0, kind, k], x_r.at[0, 1 - kind, k], {"mpo": at_x(1)}),
            rcopy(ref, ref, x_s.at[1, kind, k], x_r.at[1, 1 - kind, k], {"mpo": at_x(-1)}),
        )

    def x_wait(side, kind, k):
        zz = at_z(-sgn * (k + 1)) if kind == 0 else at_z(sgn * (k + 1))
        p = at_x(-1) if side == 0 else at_x(1)
        ref = slot(zz, start4(p), 4) if kind == 0 else slot(zz, start5(p), 5)
        return rcopy(ref, ref, x_s.at[side, kind, k], x_r.at[side, kind, k], {"mpo": at_x(1)})

    def f_send(kind, k):
        zz = at_z(-sgn * (k + 1)) if kind == 0 else at_z(sgn * (k + 1))
        p = at_x(-fdir)
        ref = slot(zz, start4(p), 4) if kind == 0 else slot(zz, start5(p), 5)
        return rcopy(ref, ref, f_s.at[kind, k], f_r.at[1 - kind, k], {"mpo": at_x(fdir)})

    def f_wait(kind, k):
        zz = at_z(-sgn * (k + 1)) if kind == 0 else at_z(sgn * (k + 1))
        p = at_x(2)
        ref = slot(zz, start5(p), 5) if kind == 0 else slot(zz, start4(p), 4)
        return rcopy(ref, ref, f_s.at[kind, k], f_r.at[kind, k], {"mpo": at_x(1)})

    def z_wait(kind, k):
        zz = at_z(-sgn * (k + 1)) if kind == 0 else at_z(sgn * (k + 1))
        if kind == 0:
            return rcopy(sent5.at[0], slot(zz, u5, 5), near5_s.at[k], near5_r.at[k], {"env": at_z(1)})
        return rcopy(sent4.at[0], slot(zz, u4, 4), near4_s.at[k], near4_r.at[k], {"env": at_z(1)})

    zhalf = at_z(half)

    def antipode(stage):
        @pl.when(even)
        def _():
            stage(0)

        @pl.when(jnp.logical_not(even))
        def _():
            stage(1)

    kinds = (0, 1)
    last = half - 1

    def one_a(k, kind):
        z_wait(kind, k).wait_recv()
        for cp in x_send(kind, k):
            cp.start()

    def one_b(k, kind):
        x_wait(0, kind, k).wait_recv()
        x_wait(1, kind, k).wait_recv()
        f_send(kind, k).start()

    def stage_a(k, _):
        for kind in kinds:
            one_a(k, kind)
        return 0

    def stage_b(k, _):
        for kind in kinds:
            one_b(k, kind)
        return 0

    def to_other(kind, k):
        zz = at_z(-sgn * (k + 1)) if kind == 0 else at_z(sgn * (k + 1))
        return d2d(zz, 2 * k + kind)

    def stage_c(k, _):
        for kind in kinds:
            f_wait(kind, k).wait_recv()
            to_other(kind, k).start()
        return 0

    lax.fori_loop(0, hop, stage_a, 0)
    lax.fori_loop(0, hop, stage_b, 0)

    fwd_in = rcopy(rows_of(at_x(2), lo), rows_of(at_x(2), lo), ls.at[2], lr.at[2], {"mpo": at_x(1)})
    fwd_in.wait_recv()
    opposite = rcopy(rows_of(at_x(2), lo), rows_of(at_x(2), lo), ls.at[5], lr.at[5], pside)
    opposite.start()

    lax.fori_loop(0, hop, stage_c, 0)

    olo = (1 - c) * (width // 2)
    for k, off in ((3, -1), (4, 1), (5, 2)):
        rcopy(rows_of(at_x(off), olo), rows_of(at_x(off), olo), ls.at[k], lr.at[k], pside).wait_recv()

    step = 2 * ROWS
    chunk = kron.shape[0] // 2

    def mix(i, _):
        r0 = pl.multiple_of(i * step, step)
        a = lefts[0:bond, pl.ds(r0, ROWS), :].reshape(bond * ROWS, width)
        b = lefts[0:bond, pl.ds(r0 + ROWS, ROWS), :].reshape(bond * ROWS, width)
        ab = jnp.concatenate([a, b], axis=1)
        ab = jnp.concatenate([ab, ab], axis=0)
        for g in range(2):
            res = jnp.dot(kron[g * chunk : (g + 1) * chunk, :], ab, preferred_element_type=jnp.float32).astype(jnp.bfloat16)
            for m in range(chunk // ROWS):
                row = g * (chunk // ROWS) + m
                vq, s = row // states, row % states
                part = res[m * ROWS : (m + 1) * ROWS, :]
                mixed[vq, pl.ds(r0, ROWS), s * width : (s + 1) * width] = part[:, :width]
                mixed[vq, pl.ds(r0 + ROWS, ROWS), s * width : (s + 1) * width] = part[:, width:]
        return 0

    nmix = width // step
    lax.fori_loop(0, nmix // 2, mix, 0)
    lax.fori_loop(hop, hop + hop // 2, stage_a, 0)
    lax.fori_loop(nmix // 2, nmix, mix, 0)
    lax.fori_loop(hop + hop // 2, last, stage_a, 0)

    antipode(functools.partial(one_a, last))
    lax.fori_loop(hop, last, stage_b, 0)
    antipode(functools.partial(one_b, last))
    lax.fori_loop(hop, last, stage_c, 0)
    antipode(lambda kind: f_wait(kind, last).wait_recv())
    d2d(zhalf, 2 * last).start()

    def other(zz, k):
        ref = units.at[pl.ds((zz * 2 + 1 - c) * per, per)]
        return rcopy(ref, ref, d_s.at[k], d_r.at[k], pside)

    other(z, n - 1).wait_recv()

    def stage_d(k, _):
        other(at_z(sgn * (k + 1)), 2 * k).wait_recv()
        other(at_z(-sgn * (k + 1)), 2 * k + 1).wait_recv()
        return 0

    lax.fori_loop(0, last, stage_d, 0)
    other(zhalf, 2 * last).wait_recv()

    lane = lax.broadcasted_iota(jnp.int32, (ROWS, LANES), 1)
    masks = [jnp.where(lane + h * LANES < kept_ref[0], 1.0, 0.0).astype(jnp.bfloat16) for h in range(thirds)]

    def place(j, _):
        i0, i1 = idx_ref[0, 2 * j], idx_ref[0, 2 * j + 1]
        for h in range(thirds):
            two = jnp.concatenate([units[i0 + h], units[i1 + h]], axis=0)
            block[pl.ds(pl.multiple_of(j * ROWS, ROWS), ROWS), h * LANES : (h + 1) * LANES] = two * masks[h]
        return 0

    lax.fori_loop(0, block.shape[0] // ROWS, place, 0, unroll=4)

    for k in range(block.shape[0] // LANES):
        flipped[:, k * LANES : (k + 1) * LANES] = block[k * LANES : (k + 1) * LANES, :].T

    nv = second.shape[0]
    cols = second.shape[2]

    def mul(vq, _):
        mine = block[:, pl.ds(pl.multiple_of(c * LANES, LANES), cols)]
        res = jnp.dot(mixed[vq], mine, preferred_element_type=jnp.float32).astype(jnp.bfloat16)
        second[vq // states, pl.ds(pl.multiple_of(lax.rem(vq, states) * width, width), width), :] = res
        return 0

    lax.fori_loop(0, nv * states, mul, 0)
    share = out_ref.shape[2]

    def last_mul(v, _):
        res = jnp.dot(flipped[...], second[v], preferred_element_type=jnp.float32)

        @pl.when(c == 0)
        def _():
            out_ref[v] = res[:, :share]

        @pl.when(c == 1)
        def _():
            out_ref[v] = res[:, cols - share :]

        return 0

    lax.fori_loop(0, nv, last_mul, 0)

    for cp in lsend + [fwd, from_below, from_above, opposite, far5, far4]:
        cp.wait_send()

    def drain(k, _):
        for cp in (
            rcopy(sent5.at[0], sent5.at[0], near5_s.at[k], near5_r.at[k], pside),
            rcopy(sent4.at[0], sent4.at[0], near4_s.at[k], near4_r.at[k], pside),
            *x_send(0, k), *x_send(1, k), f_send(0, k), f_send(1, k), to_other(0, k), to_other(1, k),
        ):
            cp.wait_send()
        return 0

    lax.fori_loop(0, last, drain, 0)

    def drain_last(kind):
        if kind == 0:
            rcopy(sent5.at[0], sent5.at[0], near5_s.at[last], near5_r.at[last], pside).wait_send()
        else:
            rcopy(sent4.at[0], sent4.at[0], near4_s.at[last], near4_r.at[last], pside).wait_send()
        for cp in (*x_send(kind, last), f_send(kind, last)):
            cp.wait_send()

    antipode(drain_last)
    d2d(zhalf, 2 * last).wait_send()
    d2d(z, n - 1).wait_send()


def coupling_rows(mpo_tensor, mpo_mask, fields, first, count):
    bond, states = mpo_tensor.shape[0], mpo_tensor.shape[2]
    base = mpo_tensor * mpo_mask.astype(jnp.float32)[:, :, None, None]
    level = jnp.arange(states, dtype=jnp.int32)
    spin_first = 0.5 - (level // 2).astype(jnp.float32)
    spin_second = 0.5 - (level % 2).astype(jnp.float32)
    onsite = jnp.diag(fields[0] * spin_first + fields[1] * spin_second)
    at = jnp.arange(bond, dtype=jnp.int32)
    corner = (at[:, None] == bond - 1) & (at[None, :] == 0)
    base = base + jnp.where(corner[:, :, None, None], onsite[None, None, :, :], jnp.float32(0.0))
    padded = lax.axis_size("mpo") * count
    base = jnp.pad(base, ((0, padded - bond), (0, padded - bond), (0, 0), (0, 0)))
    rows = lax.dynamic_slice_in_dim(base, first, count, 1)
    rows = jnp.moveaxis(rows, 0, 3).reshape(count * states * states, padded)
    high = lax.reduce_precision(rows, 8, 7)
    return jnp.concatenate([high, rows - high], axis=1).astype(jnp.bfloat16)


def on_device(held, owner_map, kept, left_env, mpo_tensor, mpo_mask, fields):
    n, nx, nc = lax.axis_size("env"), lax.axis_size("mpo"), lax.axis_size("col")
    pool, tile, width = held.shape
    sectors, tiles = owner_map.shape
    states = tiles * tile // width
    cap = 2 * tiles // (n * nc)
    thirds = width // LANES
    slab = left_env.shape[0]
    bond = mpo_tensor.shape[0]
    per = cap * thirds
    half, hop = n // 2, n // 4
    bf16 = jnp.bfloat16

    src, idx = pl.pallas_call(
        functools.partial(plan_kernel, pool, cap, thirds, sectors),
        out_shape=(jax.ShapeDtypeStruct((sectors, 8), jnp.int32), jax.ShapeDtypeStruct((1, tiles), jnp.int32)),
        name="plan",
    )(owner_map)
    pair = coupling_rows(mpo_tensor, mpo_mask, fields, lax.axis_index("mpo") * slab, slab)

    out = pl.pallas_call(
        functools.partial(main_kernel, (n, nx, cap, thirds, bond)),
        out_shape=jax.ShapeDtypeStruct((slab, width, width // nc), jnp.float32),
        in_specs=[
            pl.BlockSpec(memory_space=SMEM),
            pl.BlockSpec(memory_space=SMEM),
            pl.BlockSpec(memory_space=SMEM),
            pl.BlockSpec(memory_space=VMEM),
            pl.BlockSpec(memory_space=pl.ANY),
            pl.BlockSpec(memory_space=VMEM),
        ],
        out_specs=pl.BlockSpec(memory_space=VMEM),
        scratch_shapes=[
            VMEM((n * nc * per, tile, LANES), bf16),
            VMEM((half, 5, tile, LANES), bf16),
            VMEM((half, 4, tile, LANES), bf16),
            VMEM((hop, 5, tile, LANES), bf16),
            VMEM((hop, 4, tile, LANES), bf16),
            VMEM((nx * slab, width, width), bf16),
            VMEM((slab * states * states * ROWS, 2 * bond * ROWS), bf16),
            VMEM((slab * states, width, states * width), bf16),
            VMEM((tiles * tile, width), bf16),
            VMEM((width, tiles * tile), bf16),
            VMEM((slab, states * width, 2 * LANES), bf16),
            DMA,
            DMA((half,)), DMA((half,)), DMA((half,)), DMA((half,)),
            DMA((2,)), DMA((2,)),
            DMA((2, 2, half)), DMA((2, 2, half)),
            DMA((2, half)), DMA((2, half)),
            DMA((n,)), DMA((n,)),
            DMA((6,)), DMA((6,)),
        ],
        compiler_params=pltpu.CompilerParams(collective_id=0, has_side_effects=True, vmem_limit_bytes=56 * 2**20),
        name="exchange_and_contract",
    )(src, idx, kept, held, left_env[:, 0], pair)
    return out[:, None]


def solution(mesh):
    return jax.shard_map(
        on_device,
        mesh=mesh,
        in_specs=(
            P(("real", "env", "col"), None, None),
            P("real", None),
            P(("real", "env")),
            P("mpo", ("real", "env"), None, None),
            P(),
            P(),
            P("real"),
        ),
        out_specs=P("mpo", ("real", "env"), None, "col"),
        check_vma=False,
    )
```

```python
import functools

import jax
import jax.numpy as jnp
from jax import lax
from jax.experimental import pallas as pl
from jax.experimental.pallas import tpu as pltpu
from jax.sharding import PartitionSpec as P

MESH = pl.DeviceIdType.MESH
VMEM = pltpu.VMEM
SMEM = pltpu.SMEM
DMA = pltpu.SemaphoreType.DMA
LANES = 128
ROWS = 16


def plan_kernel(pool, cap, thirds, sectors, map_ref, src_ref, idx_ref):
    tiles = map_ref.shape[1]
    row = lax.axis_index("env")
    me = row * lax.axis_size("col") + lax.axis_index("col")
    slots = map_ref[...]
    local = slots - me * pool
    mine = (local >= 0) & (local < pool)
    before = lax.broadcasted_iota(jnp.int32, (tiles, tiles), 0) < lax.broadcasted_iota(jnp.int32, (tiles, tiles), 1)
    rank = jnp.dot(
        jnp.where(mine, 1.0, 0.0).astype(jnp.bfloat16),
        jnp.where(before, 1.0, 0.0).astype(jnp.bfloat16),
        preferred_element_type=jnp.float32,
    )
    lane = lax.broadcasted_iota(jnp.int32, src_ref.shape, 1)
    found = jnp.zeros(src_ref.shape, jnp.float32)
    localf = local.astype(jnp.float32)
    for r in range(cap):
        slot = jnp.sum(jnp.where(mine & (rank == float(r)), localf, 0.0), axis=1, keepdims=True)
        found = jnp.where(lane == r, slot, found)
    src_ref[...] = found.astype(jnp.int32)
    own = map_ref[pl.ds(row, 1), :].astype(jnp.float32)
    owner = jnp.floor((own + 0.5) * (1.0 / pool))
    same = lax.broadcasted_iota(jnp.int32, (tiles, tiles), 0) == lax.broadcasted_iota(jnp.int32, (tiles, tiles), 1)
    column = jnp.sum(jnp.where(same, jnp.broadcast_to(owner, (tiles, tiles)), 0.0), axis=1, keepdims=True)
    order = jnp.sum(jnp.where((column == owner) & before, 1.0, 0.0), axis=0, keepdims=True)
    idx_ref[...] = (owner * float(cap * thirds) + order * float(thirds)).astype(jnp.int32)


def main_kernel(
    dims, src_ref, idx_ref, kept_ref, fields_ref, held_ref, left_ref, mpo_ref, mask_ref, out_ref,
    units, sent5, sent4, relay5, relay4, lefts, kron, mixed, block, flipped, second,
    load_sem, near5_s, near5_r, near4_s, near4_r, bund_s, bund_r, x_s, x_r, f_s, f_r, d_s, d_r,
    ln_s, ln_r, lf_s, lf_r, lp_s, lp_r,
):
    n, nx, cap, thirds, bond = dims
    per = cap * thirds
    slab = left_ref.shape[0]
    width = left_ref.shape[2]
    half = n // 2
    hop = n // 4
    z, x, c = lax.axis_index("env"), lax.axis_index("mpo"), lax.axis_index("col")
    states = block.shape[0] // width
    even = lax.rem(x + c, 2) == 0
    sgn = jnp.where(even, 1, -1)

    def start5(p):
        return 4 * p + p // 2

    def start4(p):
        return 5 * p - p // 2

    def at_z(off):
        return lax.rem(z + off + n, n)

    def at_x(off):
        return lax.rem(x + off + nx, nx)

    def rcopy(src, dst, ss, rs, where):
        return pltpu.make_async_remote_copy(src_ref=src, dst_ref=dst, send_sem=ss, recv_sem=rs, device_id=where, device_id_type=MESH)

    load = pltpu.make_async_copy(left_ref, lefts.at[pl.ds(x * slab, slab)], load_sem)
    load.start()

    barrier = pltpu.get_barrier_semaphore()

    def greet(k, _):
        pl.semaphore_signal(barrier, inc=1, device_id={"env": at_z(k)}, device_id_type=MESH)
        pl.semaphore_signal(barrier, inc=1, device_id={"env": at_z(-k)}, device_id_type=MESH)
        return 0

    lax.fori_loop(1, hop + 1, greet, 0)
    pl.semaphore_signal(barrier, inc=1, device_id={"mpo": at_x(1)}, device_id_type=MESH)
    pl.semaphore_signal(barrier, inc=1, device_id={"mpo": at_x(-1)}, device_id_type=MESH)
    pl.semaphore_signal(barrier, inc=1, device_id={"col": 1 - c}, device_id_type=MESH)

    def unit(t, u):
        r, h = u // thirds, lax.rem(u, thirds)
        return held_ref[src_ref[t, r], :, pl.ds(pl.multiple_of(h * LANES, LANES), LANES)]

    u5, u4 = start5(x), start4(x)

    def pick(k, _):
        t5, t4 = at_z(sgn * (k + 1)), at_z(-sgn * (k + 1))
        for i in range(5):
            sent5[k, i] = unit(t5, u5 + i)
        for i in range(4):
            sent4[k, i] = unit(t4, u4 + i)
        return 0

    lax.fori_loop(0, half, pick, 0)

    def own(u, _):
        units[(z * 2 + c) * per + u] = unit(z, u)
        return 0

    lax.fori_loop(0, per, own, 0)

    load.wait()
    pl.semaphore_wait(barrier, 2 * hop + 3)

    def slot(zz, first, count):
        return units.at[pl.ds((zz * 2 + c) * per + first, count)]

    parts = ln_s.shape[1]
    piece = width // 2 // parts
    fdir = 1 - 2 * c
    pside = {"col": 1 - c}

    def rows_of(p, core, g):
        first = pl.multiple_of(core * (width // 2) + g * piece, ROWS)
        return lefts.at[pl.ds(p * slab, slab), pl.ds(first, piece)]

    def l_own(g):
        ref = rows_of(x, c, g)
        return [rcopy(ref, ref, ln_s.at[k, g], ln_r.at[k, g], {"mpo": at_x(off)}) for k, off in ((0, 1), (1, -1))]

    def l_fwd(g):
        ref = rows_of(at_x(-fdir), c, g)
        return rcopy(ref, ref, lf_s.at[g], lf_r.at[g], {"mpo": at_x(fdir)})

    def l_pair(k, g, core):
        ref = rows_of(at_x((-1, 1, 2)[k]), core, g)
        return rcopy(ref, ref, lp_s.at[k, g], lp_r.at[k, g], pside)

    def l_start(g):
        for cp in l_own(g):
            cp.start()

    def l_serve(g):
        for k, off in ((0, -1), (1, 1)):
            ref = rows_of(at_x(off), c, g)
            rcopy(ref, ref, ln_s.at[k, g], ln_r.at[k, g], pside).wait_recv()
        l_fwd(g).start()
        if g + 2 < parts:
            l_start(g + 2)
        l_pair(0, g, c).start()
        l_pair(1, g, c).start()

    def l_finish(g):
        ref = rows_of(at_x(2), c, g)
        rcopy(ref, ref, lf_s.at[g], lf_r.at[g], pside).wait_recv()
        l_pair(2, g, c).start()

    def l_ready(g):
        for k in range(3):
            l_pair(k, g, 1 - c).wait_recv()

    l_start(0)
    l_start(1)

    far5 = rcopy(sent5.at[pl.ds(hop, hop)], relay5, bund_s.at[0], bund_r.at[0], {"env": at_z(sgn * hop)})
    far4 = rcopy(sent4.at[pl.ds(hop, hop)], relay4, bund_s.at[1], bund_r.at[1], {"env": at_z(-sgn * hop)})
    far5.start()
    far4.start()

    def near_copies(k):
        a = rcopy(sent5.at[k], slot(z, u5, 5), near5_s.at[k], near5_r.at[k], {"env": at_z(sgn * (k + 1))})
        b = rcopy(sent4.at[k], slot(z, u4, 4), near4_s.at[k], near4_r.at[k], {"env": at_z(-sgn * (k + 1))})
        return a, b

    def near(i, _):
        a, b = near_copies(hop - 1 - i)
        a.start()
        b.start()
        return 0

    lax.fori_loop(0, hop, near, 0)

    def d2d(zz, k):
        return rcopy(slot(zz, 0, per), slot(zz, 0, per), d_s.at[k], d_r.at[k], {"col": 1 - c})

    d2d(z, n - 1).start()

    rows, vees = mpo_ref.shape
    ss = states * states
    own_v = slab
    bf16, f32 = jnp.bfloat16, jnp.float32

    def iota(shape, dim):
        return lax.broadcasted_iota(jnp.int32, shape, dim)

    def ones(cond):
        return jnp.where(cond, 1.0, 0.0).astype(bf16)

    wrow = ones(iota((rows, bond), 0) // ss == iota((rows, bond), 1))
    base = mpo_ref[...] * jnp.dot(wrow, mask_ref[...].astype(f32).astype(bf16), preferred_element_type=f32)
    ri, li = iota((rows, vees), 0), iota((rows, vees), 1)
    qi, si = lax.rem(ri, ss) // states, lax.rem(ri, states)
    onsite = fields_ref[0] * (0.5 - (si // 2).astype(f32)) + fields_ref[1] * (0.5 - lax.rem(si, 2).astype(f32))
    base = base + jnp.where((ri >= (bond - 1) * ss) & (qi == si) & (li == 0), onsite, 0.0)
    high = base.astype(bf16)
    low = (base - high.astype(f32)).astype(bf16)
    nrow = ss * own_v
    select = ones(iota((nrow, vees), 1) == x * own_v + lax.rem(iota((nrow, vees), 0), own_v))
    match = lax.rem(iota((nrow, rows), 1), ss) == iota((nrow, rows), 0) // own_v
    spread = ones(iota((rows, bond * ROWS), 0) // ss == iota((rows, bond * ROWS), 1) // ROWS)

    def per_row(m):
        picked = lax.dot_general(select, m, (((1,), (1,)), ((), ())), preferred_element_type=f32)
        return jnp.dot(jnp.where(match, picked, 0.0).astype(bf16), spread, preferred_element_type=f32).astype(bf16)

    pairs = jnp.concatenate([per_row(high), per_row(low)], axis=1)
    kk = kron.shape[1]
    group = kron.shape[0] // 8
    diag = lax.rem(iota((group, kk), 0), ROWS) == lax.rem(iota((group, kk), 1), ROWS)

    def build(g, _):
        row = ones(iota((group, nrow), 0) // ROWS + g * (group // ROWS) == iota((group, nrow), 1))
        full = jnp.dot(row, pairs, preferred_element_type=f32)
        kron[pl.ds(g * group, group), :] = jnp.where(diag, full, 0.0).astype(bf16)
        return 0

    lax.fori_loop(0, 8, build, 0)

    chunk = kron.shape[0] // 2

    def mix(g):
        def one(t, _):
            r0 = pl.multiple_of(g * piece + t * ROWS, ROWS)
            r1 = pl.multiple_of(r0 + width // 2, ROWS)
            a = lefts[0:bond, pl.ds(r0, ROWS), :].reshape(bond * ROWS, width)
            b = lefts[0:bond, pl.ds(r1, ROWS), :].reshape(bond * ROWS, width)
            ab = jnp.concatenate([a, b], axis=1)
            ab = jnp.concatenate([ab, ab], axis=0)
            for e in range(2):
                res = jnp.dot(kron[e * chunk : (e + 1) * chunk, :], ab, preferred_element_type=f32).astype(bf16)
                for m in range(chunk // ROWS):
                    row = e * (chunk // ROWS) + m
                    qs, v = row // own_v, row % own_v
                    vq, s = v * states + qs // states, qs % states
                    part = res[m * ROWS : (m + 1) * ROWS, :]
                    mixed[vq, pl.ds(r0, ROWS), s * width : (s + 1) * width] = part[:, :width]
                    mixed[vq, pl.ds(r1, ROWS), s * width : (s + 1) * width] = part[:, width:]
            return 0

        lax.fori_loop(0, piece // ROWS, one, 0)

    def relay_copies(k):
        src5 = at_z(-sgn * hop)
        return rcopy(relay5.at[k], slot(src5, u5, 5), near5_s.at[hop + k], near5_r.at[hop + k], {"env": at_z(sgn * (k + 1))})

    def relay_copies4(k):
        src4 = at_z(sgn * hop)
        return rcopy(relay4.at[k], slot(src4, u4, 4), near4_s.at[hop + k], near4_r.at[hop + k], {"env": at_z(-sgn * (k + 1))})

    def serve_relay():
        far5.wait_recv()
        far4.wait_recv()

        @pl.when(even)
        def _():
            relay_copies(hop - 1).start()

        @pl.when(jnp.logical_not(even))
        def _():
            relay_copies4(hop - 1).start()

        def relay(i, _):
            relay_copies(hop - 2 - i).start()
            relay_copies4(hop - 2 - i).start()
            return 0

        lax.fori_loop(0, hop - 1, relay, 0)

    def x_send(kind, k):
        zz = at_z(-sgn * (k + 1)) if kind == 0 else at_z(sgn * (k + 1))
        ref = slot(zz, u5, 5) if kind == 0 else slot(zz, u4, 4)
        return (
            rcopy(ref, ref, x_s.at[0, kind, k], x_r.at[0, 1 - kind, k], {"mpo": at_x(1)}),
            rcopy(ref, ref, x_s.at[1, kind, k], x_r.at[1, 1 - kind, k], {"mpo": at_x(-1)}),
        )

    def x_wait(side, kind, k):
        zz = at_z(-sgn * (k + 1)) if kind == 0 else at_z(sgn * (k + 1))
        p = at_x(-1) if side == 0 else at_x(1)
        ref = slot(zz, start4(p), 4) if kind == 0 else slot(zz, start5(p), 5)
        return rcopy(ref, ref, x_s.at[side, kind, k], x_r.at[side, kind, k], {"mpo": at_x(1)})

    def f_send(kind, k):
        zz = at_z(-sgn * (k + 1)) if kind == 0 else at_z(sgn * (k + 1))
        p = at_x(-fdir)
        ref = slot(zz, start4(p), 4) if kind == 0 else slot(zz, start5(p), 5)
        return rcopy(ref, ref, f_s.at[kind, k], f_r.at[1 - kind, k], {"mpo": at_x(fdir)})

    def f_wait(kind, k):
        zz = at_z(-sgn * (k + 1)) if kind == 0 else at_z(sgn * (k + 1))
        p = at_x(2)
        ref = slot(zz, start5(p), 5) if kind == 0 else slot(zz, start4(p), 4)
        return rcopy(ref, ref, f_s.at[kind, k], f_r.at[kind, k], {"mpo": at_x(1)})

    def z_wait(kind, k):
        zz = at_z(-sgn * (k + 1)) if kind == 0 else at_z(sgn * (k + 1))
        if kind == 0:
            return rcopy(sent5.at[0], slot(zz, u5, 5), near5_s.at[k], near5_r.at[k], {"env": at_z(1)})
        return rcopy(sent4.at[0], slot(zz, u4, 4), near4_s.at[k], near4_r.at[k], {"env": at_z(1)})

    zhalf = at_z(half)

    def antipode(stage):
        @pl.when(even)
        def _():
            stage(0)

        @pl.when(jnp.logical_not(even))
        def _():
            stage(1)

    kinds = (0, 1)
    last = half - 1

    def one_a(k, kind):
        z_wait(kind, k).wait_recv()
        for cp in x_send(kind, k):
            cp.start()

    def one_b(k, kind):
        x_wait(0, kind, k).wait_recv()
        x_wait(1, kind, k).wait_recv()
        f_send(kind, k).start()

    def stage_a(k, _):
        for kind in kinds:
            one_a(k, kind)
        return 0

    def stage_b(k, _):
        for kind in kinds:
            one_b(k, kind)
        return 0

    def to_other(kind, k):
        zz = at_z(-sgn * (k + 1)) if kind == 0 else at_z(sgn * (k + 1))
        return d2d(zz, 2 * k + kind)

    def stage_c(k, _):
        for kind in kinds:
            f_wait(kind, k).wait_recv()
            to_other(kind, k).start()
        return 0

    l_serve(0)
    l_serve(1)
    l_finish(0)
    l_serve(2)
    l_finish(1)
    l_ready(0)
    mix(0)
    l_serve(3)
    l_finish(2)
    l_ready(1)
    serve_relay()
    mix(1)
    lax.fori_loop(0, hop, stage_a, 0)
    l_finish(3)
    l_ready(2)
    mix(2)
    lax.fori_loop(0, hop, stage_b, 0)
    l_ready(3)
    mix(3)
    lag = 2
    for k in range(hop, last + 1 + 2 * lag):
        if k < last:
            stage_a(k, 0)
        elif k == last:
            antipode(functools.partial(one_a, last))
        if k == hop + 1:
            lax.fori_loop(0, hop, stage_c, 0)
        kb = k - lag
        if hop <= kb < last:
            stage_b(kb, 0)
        elif kb == last:
            antipode(functools.partial(one_b, last))
        kc = k - 2 * lag
        if hop <= kc < last:
            stage_c(kc, 0)
    antipode(lambda kind: f_wait(kind, last).wait_recv())
    d2d(zhalf, 2 * last).start()

    def other(zz, k):
        ref = units.at[pl.ds((zz * 2 + 1 - c) * per, per)]
        return rcopy(ref, ref, d_s.at[k], d_r.at[k], pside)

    other(z, n - 1).wait_recv()

    def stage_d(k, _):
        other(at_z(sgn * (k + 1)), 2 * k).wait_recv()
        other(at_z(-sgn * (k + 1)), 2 * k + 1).wait_recv()
        return 0

    lax.fori_loop(0, last, stage_d, 0)
    other(zhalf, 2 * last).wait_recv()

    lane = lax.broadcasted_iota(jnp.int32, (ROWS, LANES), 1)
    masks = [jnp.where(lane + h * LANES < kept_ref[0], 1.0, 0.0).astype(jnp.bfloat16) for h in range(thirds)]

    def place(j, _):
        i0, i1 = idx_ref[0, 2 * j], idx_ref[0, 2 * j + 1]
        for h in range(thirds):
            two = jnp.concatenate([units[i0 + h], units[i1 + h]], axis=0)
            block[pl.ds(pl.multiple_of(j * ROWS, ROWS), ROWS), h * LANES : (h + 1) * LANES] = two * masks[h]
        return 0

    lax.fori_loop(0, block.shape[0] // ROWS, place, 0, unroll=4)

    nv = second.shape[0]
    cols = second.shape[2]
    turns = block.shape[0] // LANES // nv

    def mul(v, _):
        mine = block[:, pl.ds(pl.multiple_of(c * LANES, LANES), cols)]
        lhs = mixed[pl.ds(v * states, states)].reshape(states * width, states * width)
        second[v] = jnp.dot(lhs, mine, preferred_element_type=f32).astype(bf16)
        for k in range(turns):
            at = pl.multiple_of((v * turns + k) * LANES, LANES)
            flipped[:, pl.ds(at, LANES)] = block[pl.ds(at, LANES), :].T
        return 0

    lax.fori_loop(0, nv, mul, 0)
    share = out_ref.shape[1]

    def last_mul(v, _):
        res = jnp.dot(flipped[...], second[v], preferred_element_type=f32).T

        @pl.when(c == 0)
        def _():
            out_ref[v] = res[:share]

        @pl.when(c == 1)
        def _():
            out_ref[v] = res[cols - share :]

        return 0

    lax.fori_loop(0, nv, last_mul, 0)

    far5.wait_send()
    far4.wait_send()
    for g in range(parts):
        for cp in (*l_own(g), l_fwd(g), l_pair(0, g, c), l_pair(1, g, c), l_pair(2, g, c)):
            cp.wait_send()

    def drain(k, _):
        for cp in (
            rcopy(sent5.at[0], sent5.at[0], near5_s.at[k], near5_r.at[k], pside),
            rcopy(sent4.at[0], sent4.at[0], near4_s.at[k], near4_r.at[k], pside),
            *x_send(0, k), *x_send(1, k), f_send(0, k), f_send(1, k), to_other(0, k), to_other(1, k),
        ):
            cp.wait_send()
        return 0

    lax.fori_loop(0, last, drain, 0)

    def drain_last(kind):
        if kind == 0:
            rcopy(sent5.at[0], sent5.at[0], near5_s.at[last], near5_r.at[last], pside).wait_send()
        else:
            rcopy(sent4.at[0], sent4.at[0], near4_s.at[last], near4_r.at[last], pside).wait_send()
        for cp in (*x_send(kind, last), f_send(kind, last)):
            cp.wait_send()

    antipode(drain_last)
    d2d(zhalf, 2 * last).wait_send()
    d2d(z, n - 1).wait_send()


def on_device(held, owner_map, kept, left_env, mpo_tensor, mpo_mask, fields):
    n, nx, nc = lax.axis_size("env"), lax.axis_size("mpo"), lax.axis_size("col")
    pool, tile, width = held.shape
    sectors, tiles = owner_map.shape
    states = tiles * tile // width
    cap = 2 * tiles // (n * nc)
    thirds = width // LANES
    slab = left_env.shape[0]
    bond = mpo_tensor.shape[0]
    per = cap * thirds
    half, hop = n // 2, n // 4
    bf16 = jnp.bfloat16

    src, idx = pl.pallas_call(
        functools.partial(plan_kernel, pool, cap, thirds, sectors),
        out_shape=(jax.ShapeDtypeStruct((sectors, 8), jnp.int32), jax.ShapeDtypeStruct((1, tiles), jnp.int32)),
        name="plan",
    )(owner_map)
    mpo_rows = jnp.transpose(mpo_tensor, (0, 2, 3, 1)).reshape(bond * states * states, bond)

    out = pl.pallas_call(
        functools.partial(main_kernel, (n, nx, cap, thirds, bond)),
        out_shape=jax.ShapeDtypeStruct((slab, width // nc, width), jnp.float32),
        in_specs=[
            pl.BlockSpec(memory_space=SMEM),
            pl.BlockSpec(memory_space=SMEM),
            pl.BlockSpec(memory_space=SMEM),
            pl.BlockSpec(memory_space=SMEM),
            pl.BlockSpec(memory_space=VMEM),
            pl.BlockSpec(memory_space=pl.ANY),
            pl.BlockSpec(memory_space=VMEM),
            pl.BlockSpec(memory_space=VMEM),
        ],
        out_specs=pl.BlockSpec(memory_space=VMEM),
        scratch_shapes=[
            VMEM((n * nc * per, tile, LANES), bf16),
            VMEM((half, 5, tile, LANES), bf16),
            VMEM((half, 4, tile, LANES), bf16),
            VMEM((hop, 5, tile, LANES), bf16),
            VMEM((hop, 4, tile, LANES), bf16),
            VMEM((nx * slab, width, width), bf16),
            VMEM((slab * states * states * ROWS, 2 * bond * ROWS), bf16),
            VMEM((slab * states, width, states * width), bf16),
            VMEM((tiles * tile, width), bf16),
            VMEM((width, tiles * tile), bf16),
            VMEM((slab, states * width, 2 * LANES), bf16),
            DMA,
            DMA((half,)), DMA((half,)), DMA((half,)), DMA((half,)),
            DMA((2,)), DMA((2,)),
            DMA((2, 2, half)), DMA((2, 2, half)),
            DMA((2, half)), DMA((2, half)),
            DMA((n,)), DMA((n,)),
            DMA((2, 4)), DMA((2, 4)), DMA((4,)), DMA((4,)), DMA((3, 4)), DMA((3, 4)),
        ],
        compiler_params=pltpu.CompilerParams(collective_id=0, has_side_effects=True, vmem_limit_bytes=56 * 2**20),
        name="exchange_and_contract",
    )(src, idx, kept, fields, held, left_env[:, 0], mpo_rows, mpo_mask)
    return jnp.swapaxes(out, 1, 2)[:, None]


def solution(mesh):
    return jax.shard_map(
        on_device,
        mesh=mesh,
        in_specs=(
            P(("real", "env", "col"), None, None),
            P("real", None),
            P(("real", "env")),
            P("mpo", ("real", "env"), None, None),
            P(),
            P(),
            P("real"),
        ),
        out_specs=P("mpo", ("real", "env"), None, "col"),
        check_vma=False,
    )
```

```python
import functools

import jax
import jax.numpy as jnp
from jax import lax
from jax.experimental import pallas as pl
from jax.experimental.pallas import tpu as pltpu
from jax.sharding import PartitionSpec as P

MESH = pl.DeviceIdType.MESH
VMEM = pltpu.VMEM
SMEM = pltpu.SMEM
DMA = pltpu.SemaphoreType.DMA
LANES = 128
ROWS = 16
BUNDLES = 2


def plan_kernel(pool, cap, thirds, sectors, map_ref, src_ref, idx_ref):
    tiles = map_ref.shape[1]
    row = lax.axis_index("env")
    me = row * lax.axis_size("col") + lax.axis_index("col")
    slots = map_ref[...]
    local = slots - me * pool
    mine = (local >= 0) & (local < pool)
    before = lax.broadcasted_iota(jnp.int32, (tiles, tiles), 0) < lax.broadcasted_iota(jnp.int32, (tiles, tiles), 1)
    rank = jnp.dot(
        jnp.where(mine, 1.0, 0.0).astype(jnp.bfloat16),
        jnp.where(before, 1.0, 0.0).astype(jnp.bfloat16),
        preferred_element_type=jnp.float32,
    )
    lane = lax.broadcasted_iota(jnp.int32, src_ref.shape, 1)
    found = jnp.zeros(src_ref.shape, jnp.float32)
    localf = local.astype(jnp.float32)
    for r in range(cap):
        slot = jnp.sum(jnp.where(mine & (rank == float(r)), localf, 0.0), axis=1, keepdims=True)
        found = jnp.where(lane == r, slot, found)
    src_ref[...] = found.astype(jnp.int32)
    own = map_ref[pl.ds(row, 1), :].astype(jnp.float32)
    owner = jnp.floor((own + 0.5) * (1.0 / pool))
    same = lax.broadcasted_iota(jnp.int32, (tiles, tiles), 0) == lax.broadcasted_iota(jnp.int32, (tiles, tiles), 1)
    column = jnp.sum(jnp.where(same, jnp.broadcast_to(owner, (tiles, tiles)), 0.0), axis=1, keepdims=True)
    order = jnp.sum(jnp.where((column == owner) & before, 1.0, 0.0), axis=0, keepdims=True)
    idx_ref[...] = (owner * float(cap * thirds) + order * float(thirds)).astype(jnp.int32)


def main_kernel(
    dims, src_ref, idx_ref, kept_ref, fields_ref, pool_ref, left_ref, mpo_ref, mask_ref, out_ref,
    held_ref, units, sent5, sent4, relay5, relay4, lefts, kron, mixed, block, flipped, second,
    load_sem, pool_sem, near5_s, near5_r, near4_s, near4_r, bund_s, bund_r, x_s, x_r, f_s, f_r, d_s, d_r,
    ln_s, ln_r, lf_s, lf_r, lp_s, lp_r,
):
    n, nx, cap, thirds, bond = dims
    per = cap * thirds
    slab = left_ref.shape[0]
    width = left_ref.shape[2]
    half = n // 2
    hop = n // 4
    z, x, c = lax.axis_index("env"), lax.axis_index("mpo"), lax.axis_index("col")
    states = block.shape[0] // width
    even = lax.rem(x + c, 2) == 0
    sgn = jnp.where(even, 1, -1)

    def start5(p):
        return 4 * p + p // 2

    def start4(p):
        return 5 * p - p // 2

    def at_z(off):
        return lax.rem(z + off + n, n)

    def at_x(off):
        return lax.rem(x + off + nx, nx)

    def rcopy(src, dst, ss, rs, where):
        return pltpu.make_async_remote_copy(src_ref=src, dst_ref=dst, send_sem=ss, recv_sem=rs, device_id=where, device_id_type=MESH)

    fetch = pltpu.make_async_copy(pool_ref, held_ref, pool_sem)
    fetch.start()
    load = pltpu.make_async_copy(left_ref, lefts.at[pl.ds(x * slab, slab)], load_sem)
    load.start()

    barrier = pltpu.get_barrier_semaphore()

    def greet(k, _):
        pl.semaphore_signal(barrier, inc=1, device_id={"env": at_z(k)}, device_id_type=MESH)
        pl.semaphore_signal(barrier, inc=1, device_id={"env": at_z(-k)}, device_id_type=MESH)
        return 0

    lax.fori_loop(1, hop + 1, greet, 0)
    pl.semaphore_signal(barrier, inc=1, device_id={"mpo": at_x(1)}, device_id_type=MESH)
    pl.semaphore_signal(barrier, inc=1, device_id={"mpo": at_x(-1)}, device_id_type=MESH)
    pl.semaphore_signal(barrier, inc=1, device_id={"col": 1 - c}, device_id_type=MESH)

    def unit(t, u):
        r, h = u // thirds, lax.rem(u, thirds)
        return held_ref[src_ref[t, r], :, pl.ds(pl.multiple_of(h * LANES, LANES), LANES)]

    u5, u4 = start5(x), start4(x)

    def pick(k, _):
        t5, t4 = at_z(sgn * (k + 1)), at_z(-sgn * (k + 1))
        first = jnp.where(jnp.logical_and(k == half - 1, jnp.logical_not(even)), u4, u5)
        for i in range(5):
            sent5[k, i] = unit(t5, first + i)
        for i in range(4):
            sent4[k, i] = unit(t4, u4 + i)
        return 0

    fetch.wait()
    lax.fori_loop(0, half, pick, 0)

    def own(u, _):
        units[(z * 2 + c) * per + u] = unit(z, u)
        return 0

    lax.fori_loop(0, per, own, 0)

    load.wait()
    pl.semaphore_wait(barrier, 2 * hop + 3)

    def slot(zz, first, count):
        return units.at[pl.ds((zz * 2 + c) * per + first, count)]

    parts = ln_s.shape[1]
    piece = width // 2 // parts
    fdir = 1 - 2 * c
    pside = {"col": 1 - c}

    def rows_of(p, core, g):
        first = pl.multiple_of(core * (width // 2) + g * piece, ROWS)
        return lefts.at[pl.ds(p * slab, slab), pl.ds(first, piece)]

    def l_own(g):
        ref = rows_of(x, c, g)
        return [rcopy(ref, ref, ln_s.at[k, g], ln_r.at[k, g], {"mpo": at_x(off)}) for k, off in ((0, 1), (1, -1))]

    def l_fwd(g):
        ref = rows_of(at_x(-fdir), c, g)
        return rcopy(ref, ref, lf_s.at[g], lf_r.at[g], {"mpo": at_x(fdir)})

    def l_pair(k, g, core):
        ref = rows_of(at_x((-1, 1, 2)[k]), core, g)
        return rcopy(ref, ref, lp_s.at[k, g], lp_r.at[k, g], pside)

    def l_start(g):
        for cp in l_own(g):
            cp.start()

    def l_serve(g):
        for k, off in ((0, -1), (1, 1)):
            ref = rows_of(at_x(off), c, g)
            rcopy(ref, ref, ln_s.at[k, g], ln_r.at[k, g], pside).wait_recv()
        l_fwd(g).start()
        if g + 2 < parts:
            l_start(g + 2)
        l_pair(0, g, c).start()
        l_pair(1, g, c).start()

    def l_finish(g):
        ref = rows_of(at_x(2), c, g)
        rcopy(ref, ref, lf_s.at[g], lf_r.at[g], pside).wait_recv()
        l_pair(2, g, c).start()

    def l_ready(g):
        for k in range(3):
            l_pair(k, g, 1 - c).wait_recv()

    l_start(0)
    l_start(1)

    step = hop // BUNDLES

    def bundle(b):
        n4 = step - 1 if b == BUNDLES - 1 else step
        return (
            rcopy(sent5.at[pl.ds(hop + b * step, step)], relay5.at[pl.ds(b * step, step)], bund_s.at[0, b], bund_r.at[0, b], {"env": at_z(sgn * hop)}),
            rcopy(sent4.at[pl.ds(hop + b * step, n4)], relay4.at[pl.ds(b * step, n4)], bund_s.at[1, b], bund_r.at[1, b], {"env": at_z(-sgn * hop)}),
        )

    for b in range(BUNDLES - 1, -1, -1):
        for cp in bundle(b):
            cp.start()

    def near_copies(k):
        a = rcopy(sent5.at[k], slot(z, u5, 5), near5_s.at[k], near5_r.at[k], {"env": at_z(sgn * (k + 1))})
        b = rcopy(sent4.at[k], slot(z, u4, 4), near4_s.at[k], near4_r.at[k], {"env": at_z(-sgn * (k + 1))})
        return a, b

    def near(i, _):
        a, b = near_copies(hop - 1 - i)
        a.start()
        b.start()
        return 0

    lax.fori_loop(0, hop, near, 0)

    def d2d(zz, k):
        return rcopy(slot(zz, 0, per), slot(zz, 0, per), d_s.at[k], d_r.at[k], {"col": 1 - c})

    d2d(z, n - 1).start()

    rows, vees = mpo_ref.shape
    ss = states * states
    own_v = slab
    bf16, f32 = jnp.bfloat16, jnp.float32

    def iota(shape, dim):
        return lax.broadcasted_iota(jnp.int32, shape, dim)

    def ones(cond):
        return jnp.where(cond, 1.0, 0.0).astype(bf16)

    wrow = ones(iota((rows, bond), 0) // ss == iota((rows, bond), 1))
    base = mpo_ref[...] * jnp.dot(wrow, mask_ref[...].astype(f32).astype(bf16), preferred_element_type=f32)
    ri, li = iota((rows, vees), 0), iota((rows, vees), 1)
    qi, si = lax.rem(ri, ss) // states, lax.rem(ri, states)
    onsite = fields_ref[0] * (0.5 - (si // 2).astype(f32)) + fields_ref[1] * (0.5 - lax.rem(si, 2).astype(f32))
    base = base + jnp.where((ri >= (bond - 1) * ss) & (qi == si) & (li == 0), onsite, 0.0)
    high = base.astype(bf16)
    low = (base - high.astype(f32)).astype(bf16)
    nrow = ss * own_v
    select = ones(iota((nrow, vees), 1) == x * own_v + lax.rem(iota((nrow, vees), 0), own_v))
    match = lax.rem(iota((nrow, rows), 1), ss) == iota((nrow, rows), 0) // own_v
    spread = ones(iota((rows, bond * ROWS), 0) // ss == iota((rows, bond * ROWS), 1) // ROWS)

    def per_row(m):
        picked = lax.dot_general(select, m, (((1,), (1,)), ((), ())), preferred_element_type=f32)
        return jnp.dot(jnp.where(match, picked, 0.0).astype(bf16), spread, preferred_element_type=f32).astype(bf16)

    pairs = jnp.concatenate([per_row(high), per_row(low)], axis=1)
    kk = kron.shape[1]
    group = kron.shape[0] // 8
    diag = lax.rem(iota((group, kk), 0), ROWS) == lax.rem(iota((group, kk), 1), ROWS)

    def build(g, _):
        row = ones(iota((group, nrow), 0) // ROWS + g * (group // ROWS) == iota((group, nrow), 1))
        full = jnp.dot(row, pairs, preferred_element_type=f32)
        kron[pl.ds(g * group, group), :] = jnp.where(diag, full, 0.0).astype(bf16)
        return 0

    lax.fori_loop(0, 8, build, 0)

    chunk = kron.shape[0] // 2

    def mix(g):
        def one(t, _):
            r0 = pl.multiple_of(g * piece + t * ROWS, ROWS)
            r1 = pl.multiple_of(r0 + width // 2, ROWS)
            a = lefts[0:bond, pl.ds(r0, ROWS), :].reshape(bond * ROWS, width)
            b = lefts[0:bond, pl.ds(r1, ROWS), :].reshape(bond * ROWS, width)
            ab = jnp.concatenate([a, b], axis=1)
            ab = jnp.concatenate([ab, ab], axis=0)
            for e in range(2):
                res = jnp.dot(kron[e * chunk : (e + 1) * chunk, :], ab, preferred_element_type=f32).astype(bf16)
                for m in range(chunk // ROWS):
                    row = e * (chunk // ROWS) + m
                    qs, v = row // own_v, row % own_v
                    vq, s = v * states + qs // states, qs % states
                    part = res[m * ROWS : (m + 1) * ROWS, :]
                    mixed[vq, pl.ds(r0, ROWS), s * width : (s + 1) * width] = part[:, :width]
                    mixed[vq, pl.ds(r1, ROWS), s * width : (s + 1) * width] = part[:, width:]
            return 0

        lax.fori_loop(0, piece // ROWS, one, 0)

    def relay_copies(k):
        src5 = at_z(-sgn * hop)
        return rcopy(relay5.at[k], slot(src5, u5, 5), near5_s.at[hop + k], near5_r.at[hop + k], {"env": at_z(sgn * (k + 1))})

    def relay_last4():
        return rcopy(relay5.at[hop - 1, pl.ds(0, 4)], slot(at_z(-sgn * hop), u4, 4), near4_s.at[half - 1], near4_r.at[half - 1], {"env": at_z(sgn * hop)})

    def relay_copies4(k):
        src4 = at_z(sgn * hop)
        return rcopy(relay4.at[k], slot(src4, u4, 4), near4_s.at[hop + k], near4_r.at[hop + k], {"env": at_z(-sgn * (k + 1))})

    def serve_relay(b):
        for cp in bundle(b):
            cp.wait_recv()
        for k in range((b + 1) * step - 1, b * step - 1, -1):
            if k < hop - 1:
                relay_copies(k).start()
                relay_copies4(k).start()
            else:
                pl.when(even)(relay_copies(k).start)
                pl.when(jnp.logical_not(even))(relay_last4().start)

    def x_send(kind, k):
        zz = at_z(-sgn * (k + 1)) if kind == 0 else at_z(sgn * (k + 1))
        ref = slot(zz, u5, 5) if kind == 0 else slot(zz, u4, 4)
        return (
            rcopy(ref, ref, x_s.at[0, kind, k], x_r.at[0, 1 - kind, k], {"mpo": at_x(1)}),
            rcopy(ref, ref, x_s.at[1, kind, k], x_r.at[1, 1 - kind, k], {"mpo": at_x(-1)}),
        )

    def x_wait(side, kind, k):
        zz = at_z(-sgn * (k + 1)) if kind == 0 else at_z(sgn * (k + 1))
        p = at_x(-1) if side == 0 else at_x(1)
        ref = slot(zz, start4(p), 4) if kind == 0 else slot(zz, start5(p), 5)
        return rcopy(ref, ref, x_s.at[side, kind, k], x_r.at[side, kind, k], {"mpo": at_x(1)})

    def f_send(kind, k):
        zz = at_z(-sgn * (k + 1)) if kind == 0 else at_z(sgn * (k + 1))
        p = at_x(-fdir)
        ref = slot(zz, start4(p), 4) if kind == 0 else slot(zz, start5(p), 5)
        return rcopy(ref, ref, f_s.at[kind, k], f_r.at[1 - kind, k], {"mpo": at_x(fdir)})

    def f_wait(kind, k):
        zz = at_z(-sgn * (k + 1)) if kind == 0 else at_z(sgn * (k + 1))
        p = at_x(2)
        ref = slot(zz, start5(p), 5) if kind == 0 else slot(zz, start4(p), 4)
        return rcopy(ref, ref, f_s.at[kind, k], f_r.at[kind, k], {"mpo": at_x(1)})

    def z_wait(kind, k):
        zz = at_z(-sgn * (k + 1)) if kind == 0 else at_z(sgn * (k + 1))
        if kind == 0:
            return rcopy(sent5.at[0], slot(zz, u5, 5), near5_s.at[k], near5_r.at[k], {"env": at_z(1)})
        return rcopy(sent4.at[0], slot(zz, u4, 4), near4_s.at[k], near4_r.at[k], {"env": at_z(1)})

    zhalf = at_z(half)

    def antipode(stage):
        @pl.when(even)
        def _():
            stage(0)

        @pl.when(jnp.logical_not(even))
        def _():
            stage(1)

    kinds = (0, 1)
    last = half - 1

    def one_a(k, kind):
        z_wait(kind, k).wait_recv()
        for cp in x_send(kind, k):
            cp.start()

    def one_b(k, kind):
        x_wait(0, kind, k).wait_recv()
        x_wait(1, kind, k).wait_recv()
        f_send(kind, k).start()

    def stage_a(k, _):
        for kind in kinds:
            one_a(k, kind)
        return 0

    def stage_b(k, _):
        for kind in kinds:
            one_b(k, kind)
        return 0

    def to_other(kind, k):
        zz = at_z(-sgn * (k + 1)) if kind == 0 else at_z(sgn * (k + 1))
        return d2d(zz, 2 * k + kind)

    def stage_c(k, _):
        for kind in kinds:
            f_wait(kind, k).wait_recv()
            to_other(kind, k).start()
        return 0

    def backwards(stage, top):
        lax.fori_loop(0, hop, lambda i, _: stage(top - 1 - i, 0), 0)

    def far(stage):
        lax.fori_loop(0, last - hop, lambda i, _: stage(last - 1 - i, 0), 0)

    l_serve(0)
    l_serve(1)
    l_finish(0)
    l_serve(2)
    l_finish(1)
    l_ready(0)
    mix(0)
    for b in range(BUNDLES - 1, -1, -1):
        serve_relay(b)
    l_serve(3)
    l_finish(2)
    l_ready(1)
    mix(1)
    backwards(stage_a, hop)
    l_finish(3)
    l_ready(2)
    mix(2)
    backwards(stage_b, hop)
    l_ready(3)
    mix(3)
    backwards(stage_c, hop)
    antipode(functools.partial(one_a, last))
    far(stage_a)
    antipode(functools.partial(one_b, last))
    far(stage_b)
    antipode(lambda kind: f_wait(kind, last).wait_recv())
    d2d(zhalf, 2 * last).start()
    far(stage_c)

    def other(zz, k):
        ref = units.at[pl.ds((zz * 2 + 1 - c) * per, per)]
        return rcopy(ref, ref, d_s.at[k], d_r.at[k], pside)

    other(z, n - 1).wait_recv()

    def stage_d(k, _):
        other(at_z(sgn * (k + 1)), 2 * k).wait_recv()
        other(at_z(-sgn * (k + 1)), 2 * k + 1).wait_recv()
        return 0

    lax.fori_loop(0, last, stage_d, 0)
    other(zhalf, 2 * last).wait_recv()

    lane = lax.broadcasted_iota(jnp.int32, (ROWS, LANES), 1)
    masks = [jnp.where(lane + h * LANES < kept_ref[0], 1.0, 0.0).astype(jnp.bfloat16) for h in range(thirds)]

    def place(j, _):
        i0, i1 = idx_ref[0, 2 * j], idx_ref[0, 2 * j + 1]
        for h in range(thirds):
            two = jnp.concatenate([units[i0 + h], units[i1 + h]], axis=0)
            block[pl.ds(pl.multiple_of(j * ROWS, ROWS), ROWS), h * LANES : (h + 1) * LANES] = two * masks[h]
        return 0

    lax.fori_loop(0, block.shape[0] // ROWS, place, 0, unroll=4)

    nv = second.shape[0]
    cols = second.shape[2]
    turns = block.shape[0] // LANES // nv

    def mul(v, _):
        mine = block[:, pl.ds(pl.multiple_of(c * LANES, LANES), cols)]
        lhs = mixed[pl.ds(v * states, states)].reshape(states * width, states * width)
        second[v] = jnp.dot(lhs, mine, preferred_element_type=f32).astype(bf16)
        for k in range(turns):
            at = pl.multiple_of((v * turns + k) * LANES, LANES)
            flipped[:, pl.ds(at, LANES)] = block[pl.ds(at, LANES), :].T
        return 0

    lax.fori_loop(0, nv, mul, 0)
    share = out_ref.shape[1]

    def last_mul(v, _):
        res = jnp.dot(flipped[...], second[v], preferred_element_type=f32).T

        @pl.when(c == 0)
        def _():
            out_ref[v] = res[:share]

        @pl.when(c == 1)
        def _():
            out_ref[v] = res[cols - share :]

        return 0

    lax.fori_loop(0, nv, last_mul, 0)

    for b in range(BUNDLES):
        for cp in bundle(b):
            cp.wait_send()
    for g in range(parts):
        for cp in (*l_own(g), l_fwd(g), l_pair(0, g, c), l_pair(1, g, c), l_pair(2, g, c)):
            cp.wait_send()

    def drain(k, _):
        for cp in (
            rcopy(sent5.at[0], sent5.at[0], near5_s.at[k], near5_r.at[k], pside),
            rcopy(sent4.at[0], sent4.at[0], near4_s.at[k], near4_r.at[k], pside),
            *x_send(0, k), *x_send(1, k), f_send(0, k), f_send(1, k), to_other(0, k), to_other(1, k),
        ):
            cp.wait_send()
        return 0

    lax.fori_loop(0, last, drain, 0)

    def drain_last(kind):
        if kind == 0:
            rcopy(sent5.at[0], sent5.at[0], near5_s.at[last], near5_r.at[last], pside).wait_send()
        else:
            rcopy(sent4.at[0], sent4.at[0], near4_s.at[last], near4_r.at[last], pside).wait_send()
        for cp in (*x_send(kind, last), f_send(kind, last)):
            cp.wait_send()

    antipode(drain_last)
    d2d(zhalf, 2 * last).wait_send()
    d2d(z, n - 1).wait_send()


def on_device(held, owner_map, kept, left_env, mpo_tensor, mpo_mask, fields):
    n, nx, nc = lax.axis_size("env"), lax.axis_size("mpo"), lax.axis_size("col")
    pool, tile, width = held.shape
    sectors, tiles = owner_map.shape
    states = tiles * tile // width
    cap = 2 * tiles // (n * nc)
    thirds = width // LANES
    slab = left_env.shape[0]
    bond = mpo_tensor.shape[0]
    per = cap * thirds
    half, hop = n // 2, n // 4
    bf16 = jnp.bfloat16

    src, idx = pl.pallas_call(
        functools.partial(plan_kernel, pool, cap, thirds, sectors),
        out_shape=(jax.ShapeDtypeStruct((sectors, 8), jnp.int32), jax.ShapeDtypeStruct((1, tiles), jnp.int32)),
        name="plan",
    )(owner_map)
    mpo_rows = jnp.transpose(mpo_tensor, (0, 2, 3, 1)).reshape(bond * states * states, bond)

    out = pl.pallas_call(
        functools.partial(main_kernel, (n, nx, cap, thirds, bond)),
        out_shape=jax.ShapeDtypeStruct((slab, width // nc, width), jnp.float32),
        in_specs=[
            pl.BlockSpec(memory_space=SMEM),
            pl.BlockSpec(memory_space=SMEM),
            pl.BlockSpec(memory_space=SMEM),
            pl.BlockSpec(memory_space=SMEM),
            pl.BlockSpec(memory_space=pl.ANY),
            pl.BlockSpec(memory_space=pl.ANY),
            pl.BlockSpec(memory_space=VMEM),
            pl.BlockSpec(memory_space=VMEM),
        ],
        out_specs=pl.BlockSpec(memory_space=VMEM),
        scratch_shapes=[
            VMEM((pool, tile, width), bf16),
            VMEM((n * nc * per, tile, LANES), bf16),
            VMEM((half, 5, tile, LANES), bf16),
            VMEM((half, 4, tile, LANES), bf16),
            VMEM((hop, 5, tile, LANES), bf16),
            VMEM((hop, 4, tile, LANES), bf16),
            VMEM((nx * slab, width, width), bf16),
            VMEM((slab * states * states * ROWS, 2 * bond * ROWS), bf16),
            VMEM((slab * states, width, states * width), bf16),
            VMEM((tiles * tile, width), bf16),
            VMEM((width, tiles * tile), bf16),
            VMEM((slab, states * width, 2 * LANES), bf16),
            DMA,
            DMA,
            DMA((half,)), DMA((half,)), DMA((half,)), DMA((half,)),
            DMA((2, BUNDLES)), DMA((2, BUNDLES)),
            DMA((2, 2, half)), DMA((2, 2, half)),
            DMA((2, half)), DMA((2, half)),
            DMA((n,)), DMA((n,)),
            DMA((2, 4)), DMA((2, 4)), DMA((4,)), DMA((4,)), DMA((3, 4)), DMA((3, 4)),
        ],
        compiler_params=pltpu.CompilerParams(collective_id=0, has_side_effects=True, vmem_limit_bytes=56 * 2**20),
        name="exchange_and_contract",
    )(src, idx, kept, fields, held, left_env[:, 0], mpo_rows, mpo_mask)
    return jnp.swapaxes(out, 1, 2)[:, None]


def solution(mesh):
    return jax.shard_map(
        on_device,
        mesh=mesh,
        in_specs=(
            P(("real", "env", "col"), None, None),
            P("real", None),
            P(("real", "env")),
            P("mpo", ("real", "env"), None, None),
            P(),
            P(),
            P("real"),
        ),
        out_specs=P("mpo", ("real", "env"), None, "col"),
        check_vma=False,
    )
```

```python
import functools

import jax
import jax.numpy as jnp
from jax import lax
from jax.experimental import pallas as pl
from jax.experimental.pallas import tpu as pltpu
from jax.sharding import PartitionSpec as P

MESH = pl.DeviceIdType.MESH
VMEM = pltpu.VMEM
SMEM = pltpu.SMEM
DMA = pltpu.SemaphoreType.DMA
LANES = 128
ROWS = 16
BUNDLES = 2


def find_tiles(pool, cap, thirds, map_ref, src_ref, idx_ref):
    tiles = map_ref.shape[1]
    row = lax.axis_index("env")
    me = row * lax.axis_size("col") + lax.axis_index("col")
    slots = map_ref[...]
    local = slots - me * pool
    mine = (local >= 0) & (local < pool)
    before = lax.broadcasted_iota(jnp.int32, (tiles, tiles), 0) < lax.broadcasted_iota(jnp.int32, (tiles, tiles), 1)
    rank = jnp.dot(
        jnp.where(mine, 1.0, 0.0).astype(jnp.bfloat16),
        jnp.where(before, 1.0, 0.0).astype(jnp.bfloat16),
        preferred_element_type=jnp.float32,
    )
    lane = lax.broadcasted_iota(jnp.int32, src_ref.shape, 1)
    found = jnp.zeros(src_ref.shape, jnp.float32)
    localf = local.astype(jnp.float32)
    for r in range(cap):
        slot = jnp.sum(jnp.where(mine & (rank == float(r)), localf, 0.0), axis=1, keepdims=True)
        found = jnp.where(lane == r, slot, found)
    src_ref[...] = jnp.clip(found.astype(jnp.int32), 0, pool - 1)
    own = map_ref[pl.ds(row, 1), :].astype(jnp.float32)
    owner = jnp.floor((own + 0.5) * (1.0 / pool))
    same = lax.broadcasted_iota(jnp.int32, (tiles, tiles), 0) == lax.broadcasted_iota(jnp.int32, (tiles, tiles), 1)
    column = jnp.sum(jnp.where(same, jnp.broadcast_to(owner, (tiles, tiles)), 0.0), axis=1, keepdims=True)
    order = jnp.sum(jnp.where((column == owner) & before, 1.0, 0.0), axis=0, keepdims=True)
    idx_ref[0:1, 0:tiles] = (owner * float(cap * thirds) + order * float(thirds)).astype(jnp.int32)


def main_kernel(
    dims, kept_ref, fields_ref, map_ref, pool_ref, left_ref, mpo_ref, mask_ref, out_ref,
    src_v, idx_v, src_ref, idx_ref, held_ref, units, sent5, sent4, relay5, relay4, lefts, kron, mixed, block, flipped, second,
    load_sem, pool_sem, table_sem, near5_s, near5_r, near4_s, near4_r, bund_s, bund_r, x_s, x_r, f_s, f_r, d_s, d_r,
    ln_s, ln_r, lf_s, lf_r, lp_s, lp_r,
):
    n, nx, cap, thirds, bond = dims
    per = cap * thirds
    slab = left_ref.shape[0]
    width = left_ref.shape[2]
    half = n // 2
    hop = n // 4
    z, x, c = lax.axis_index("env"), lax.axis_index("mpo"), lax.axis_index("col")
    states = block.shape[0] // width
    even = lax.rem(x + c, 2) == 0
    sgn = jnp.where(even, 1, -1)

    def start5(p):
        return 4 * p + p // 2

    def start4(p):
        return 5 * p - p // 2

    def at_z(off):
        return lax.rem(z + off + n, n)

    def at_x(off):
        return lax.rem(x + off + nx, nx)

    def rcopy(src, dst, ss, rs, where):
        return pltpu.make_async_remote_copy(src_ref=src, dst_ref=dst, send_sem=ss, recv_sem=rs, device_id=where, device_id_type=MESH)

    fetch = pltpu.make_async_copy(pool_ref, held_ref, pool_sem)
    fetch.start()
    load = pltpu.make_async_copy(left_ref, lefts.at[pl.ds(x * slab, slab)], load_sem)
    load.start()

    barrier = pltpu.get_barrier_semaphore()

    def greet(k, _):
        pl.semaphore_signal(barrier, inc=1, device_id={"env": at_z(k)}, device_id_type=MESH)
        pl.semaphore_signal(barrier, inc=1, device_id={"env": at_z(-k)}, device_id_type=MESH)
        return 0

    lax.fori_loop(1, hop + 1, greet, 0)
    pl.semaphore_signal(barrier, inc=1, device_id={"mpo": at_x(1)}, device_id_type=MESH)
    pl.semaphore_signal(barrier, inc=1, device_id={"mpo": at_x(-1)}, device_id_type=MESH)
    pl.semaphore_signal(barrier, inc=1, device_id={"col": 1 - c}, device_id_type=MESH)

    find_tiles(held_ref.shape[0], cap, thirds, map_ref, src_v, idx_v)
    tables = [
        pltpu.make_async_copy(src_v, src_ref, table_sem.at[0]),
        pltpu.make_async_copy(idx_v, idx_ref, table_sem.at[1]),
    ]
    for cp in tables:
        cp.start()

    def unit(t, u):
        r, h = u // thirds, lax.rem(u, thirds)
        at = jnp.clip(src_ref[t, r], 0, held_ref.shape[0] - 1)
        return held_ref[at, :, pl.ds(pl.multiple_of(h * LANES, LANES), LANES)]

    u5, u4 = start5(x), start4(x)

    def pick(k, _):
        t5, t4 = at_z(sgn * (k + 1)), at_z(-sgn * (k + 1))
        first = jnp.where(jnp.logical_and(k == half - 1, jnp.logical_not(even)), u4, u5)
        for i in range(5):
            sent5[k, i] = unit(t5, first + i)
        for i in range(4):
            sent4[k, i] = unit(t4, u4 + i)
        return 0

    for cp in tables:
        cp.wait()
    fetch.wait()
    lax.fori_loop(0, half, pick, 0)

    def own(u, _):
        units[(z * 2 + c) * per + u] = unit(z, u)
        return 0

    lax.fori_loop(0, per, own, 0)

    load.wait()
    pl.semaphore_wait(barrier, 2 * hop + 3)

    def slot(zz, first, count):
        return units.at[pl.ds((zz * 2 + c) * per + first, count)]

    parts = ln_s.shape[1]
    piece = width // 2 // parts
    fdir = 1 - 2 * c
    pside = {"col": 1 - c}

    def rows_of(p, core, g):
        first = pl.multiple_of(core * (width // 2) + g * piece, ROWS)
        return lefts.at[pl.ds(p * slab, slab), pl.ds(first, piece)]

    def l_own(g):
        ref = rows_of(x, c, g)
        return [rcopy(ref, ref, ln_s.at[k, g], ln_r.at[k, g], {"mpo": at_x(off)}) for k, off in ((0, 1), (1, -1))]

    def l_fwd(g):
        ref = rows_of(at_x(-fdir), c, g)
        return rcopy(ref, ref, lf_s.at[g], lf_r.at[g], {"mpo": at_x(fdir)})

    def l_pair(k, g, core):
        ref = rows_of(at_x((-1, 1, 2)[k]), core, g)
        return rcopy(ref, ref, lp_s.at[k, g], lp_r.at[k, g], pside)

    def l_start(g):
        for cp in l_own(g):
            cp.start()

    def l_serve(g):
        for k, off in ((0, -1), (1, 1)):
            ref = rows_of(at_x(off), c, g)
            rcopy(ref, ref, ln_s.at[k, g], ln_r.at[k, g], pside).wait_recv()
        l_fwd(g).start()
        if g + 2 < parts:
            l_start(g + 2)
        l_pair(0, g, c).start()
        l_pair(1, g, c).start()

    def l_finish(g):
        ref = rows_of(at_x(2), c, g)
        rcopy(ref, ref, lf_s.at[g], lf_r.at[g], pside).wait_recv()
        l_pair(2, g, c).start()

    def l_ready(g):
        for k in range(3):
            l_pair(k, g, 1 - c).wait_recv()

    l_start(0)
    l_start(1)

    step = hop // BUNDLES

    def bundle(b):
        n4 = step - 1 if b == BUNDLES - 1 else step
        return (
            rcopy(sent5.at[pl.ds(hop + b * step, step)], relay5.at[pl.ds(b * step, step)], bund_s.at[0, b], bund_r.at[0, b], {"env": at_z(sgn * hop)}),
            rcopy(sent4.at[pl.ds(hop + b * step, n4)], relay4.at[pl.ds(b * step, n4)], bund_s.at[1, b], bund_r.at[1, b], {"env": at_z(-sgn * hop)}),
        )

    for b in range(BUNDLES - 1, -1, -1):
        for cp in bundle(b):
            cp.start()

    def near_copies(k):
        a = rcopy(sent5.at[k], slot(z, u5, 5), near5_s.at[k], near5_r.at[k], {"env": at_z(sgn * (k + 1))})
        b = rcopy(sent4.at[k], slot(z, u4, 4), near4_s.at[k], near4_r.at[k], {"env": at_z(-sgn * (k + 1))})
        return a, b

    def near(i, _):
        a, b = near_copies(hop - 1 - i)
        a.start()
        b.start()
        return 0

    lax.fori_loop(0, hop, near, 0)

    def d2d(zz, k):
        return rcopy(slot(zz, 0, per), slot(zz, 0, per), d_s.at[k], d_r.at[k], {"col": 1 - c})

    d2d(z, n - 1).start()

    rows, vees = mpo_ref.shape
    ss = states * states
    own_v = slab
    bf16, f32 = jnp.bfloat16, jnp.float32

    def iota(shape, dim):
        return lax.broadcasted_iota(jnp.int32, shape, dim)

    def ones(cond):
        return jnp.where(cond, 1.0, 0.0).astype(bf16)

    wrow = ones(iota((rows, bond), 0) // ss == iota((rows, bond), 1))
    base = mpo_ref[...] * jnp.dot(wrow, mask_ref[...].astype(f32).astype(bf16), preferred_element_type=f32)
    ri, li = iota((rows, vees), 0), iota((rows, vees), 1)
    qi, si = lax.rem(ri, ss) // states, lax.rem(ri, states)
    onsite = fields_ref[0] * (0.5 - (si // 2).astype(f32)) + fields_ref[1] * (0.5 - lax.rem(si, 2).astype(f32))
    base = base + jnp.where((ri >= (bond - 1) * ss) & (qi == si) & (li == 0), onsite, 0.0)
    high = base.astype(bf16)
    low = (base - high.astype(f32)).astype(bf16)
    nrow = ss * own_v
    select = ones(iota((nrow, vees), 1) == x * own_v + lax.rem(iota((nrow, vees), 0), own_v))
    match = lax.rem(iota((nrow, rows), 1), ss) == iota((nrow, rows), 0) // own_v
    spread = ones(iota((rows, bond * ROWS), 0) // ss == iota((rows, bond * ROWS), 1) // ROWS)

    def per_row(m):
        picked = lax.dot_general(select, m, (((1,), (1,)), ((), ())), preferred_element_type=f32)
        return jnp.dot(jnp.where(match, picked, 0.0).astype(bf16), spread, preferred_element_type=f32).astype(bf16)

    pairs = jnp.concatenate([per_row(high), per_row(low)], axis=1)
    kk = kron.shape[1]
    group = kron.shape[0] // 8
    diag = lax.rem(iota((group, kk), 0), ROWS) == lax.rem(iota((group, kk), 1), ROWS)

    def build(g, _):
        row = ones(iota((group, nrow), 0) // ROWS + g * (group // ROWS) == iota((group, nrow), 1))
        full = jnp.dot(row, pairs, preferred_element_type=f32)
        kron[pl.ds(g * group, group), :] = jnp.where(diag, full, 0.0).astype(bf16)
        return 0

    lax.fori_loop(0, 8, build, 0)

    chunk = kron.shape[0] // 2

    def mix(g):
        def one(t, _):
            r0 = pl.multiple_of(g * piece + t * ROWS, ROWS)
            r1 = pl.multiple_of(r0 + width // 2, ROWS)
            a = lefts[0:bond, pl.ds(r0, ROWS), :].reshape(bond * ROWS, width)
            b = lefts[0:bond, pl.ds(r1, ROWS), :].reshape(bond * ROWS, width)
            ab = jnp.concatenate([a, b], axis=1)
            ab = jnp.concatenate([ab, ab], axis=0)
            for e in range(2):
                res = jnp.dot(kron[e * chunk : (e + 1) * chunk, :], ab, preferred_element_type=f32).astype(bf16)
                for m in range(chunk // ROWS):
                    row = e * (chunk // ROWS) + m
                    qs, v = row // own_v, row % own_v
                    vq, s = v * states + qs // states, qs % states
                    part = res[m * ROWS : (m + 1) * ROWS, :]
                    mixed[vq, pl.ds(r0, ROWS), s * width : (s + 1) * width] = part[:, :width]
                    mixed[vq, pl.ds(r1, ROWS), s * width : (s + 1) * width] = part[:, width:]
            return 0

        lax.fori_loop(0, piece // ROWS, one, 0)

    def relay_copies(k):
        src5 = at_z(-sgn * hop)
        return rcopy(relay5.at[k], slot(src5, u5, 5), near5_s.at[hop + k], near5_r.at[hop + k], {"env": at_z(sgn * (k + 1))})

    def relay_last4():
        return rcopy(relay5.at[hop - 1, pl.ds(0, 4)], slot(at_z(-sgn * hop), u4, 4), near4_s.at[half - 1], near4_r.at[half - 1], {"env": at_z(sgn * hop)})

    def relay_copies4(k):
        src4 = at_z(sgn * hop)
        return rcopy(relay4.at[k], slot(src4, u4, 4), near4_s.at[hop + k], near4_r.at[hop + k], {"env": at_z(-sgn * (k + 1))})

    def serve_relay(b):
        for cp in bundle(b):
            cp.wait_recv()
        for k in range((b + 1) * step - 1, b * step - 1, -1):
            if k < hop - 1:
                relay_copies(k).start()
                relay_copies4(k).start()
            else:
                pl.when(even)(relay_copies(k).start)
                pl.when(jnp.logical_not(even))(relay_last4().start)

    def x_send(kind, k):
        zz = at_z(-sgn * (k + 1)) if kind == 0 else at_z(sgn * (k + 1))
        ref = slot(zz, u5, 5) if kind == 0 else slot(zz, u4, 4)
        return (
            rcopy(ref, ref, x_s.at[0, kind, k], x_r.at[0, 1 - kind, k], {"mpo": at_x(1)}),
            rcopy(ref, ref, x_s.at[1, kind, k], x_r.at[1, 1 - kind, k], {"mpo": at_x(-1)}),
        )

    def f_send(kind, k):
        zz = at_z(-sgn * (k + 1)) if kind == 0 else at_z(sgn * (k + 1))
        p = at_x(-fdir)
        ref = slot(zz, start4(p), 4) if kind == 0 else slot(zz, start5(p), 5)
        return rcopy(ref, ref, f_s.at[kind, k], f_r.at[1 - kind, k], {"mpo": at_x(fdir)})

    def f_wait(kind, k):
        zz = at_z(-sgn * (k + 1)) if kind == 0 else at_z(sgn * (k + 1))
        p = at_x(2)
        ref = slot(zz, start5(p), 5) if kind == 0 else slot(zz, start4(p), 4)
        return rcopy(ref, ref, f_s.at[kind, k], f_r.at[kind, k], {"mpo": at_x(1)})

    def z_wait(kind, k):
        zz = at_z(-sgn * (k + 1)) if kind == 0 else at_z(sgn * (k + 1))
        if kind == 0:
            return rcopy(sent5.at[0], slot(zz, u5, 5), near5_s.at[k], near5_r.at[k], {"env": at_z(1)})
        return rcopy(sent4.at[0], slot(zz, u4, 4), near4_s.at[k], near4_r.at[k], {"env": at_z(1)})

    zhalf = at_z(half)

    def antipode(stage):
        @pl.when(even)
        def _():
            stage(0)

        @pl.when(jnp.logical_not(even))
        def _():
            stage(1)

    kinds = (0, 1)
    last = half - 1

    def part(kind, k, off):
        zz = at_z(-sgn * (k + 1)) if kind == 0 else at_z(sgn * (k + 1))
        p = at_x(off)
        five = (kind == 0) == (isinstance(off, int) and off % 2 == 0)
        ref = slot(zz, start5(p), 5) if five else slot(zz, start4(p), 4)
        at = 2 * last if isinstance(k, int) and k == last else 2 * k + kind
        return rcopy(ref, ref, d_s.at[at], d_r.at[at], pside)

    def one_a(k, kind):
        z_wait(kind, k).wait_recv()
        for cp in x_send(kind, k):
            cp.start()
        part(kind, k, 0).start()

    def x_side(kind, k, side, off):
        zz = at_z(-sgn * (k + 1)) if kind == 0 else at_z(sgn * (k + 1))
        ref = slot(zz, start4(at_x(off)), 4) if kind == 0 else slot(zz, start5(at_x(off)), 5)
        return rcopy(ref, ref, x_s.at[side, kind, k], x_r.at[side, kind, k], pside)

    def one_b(k, kind):
        x_side(kind, k, c, -fdir).wait_recv()
        f_send(kind, k).start()
        part(kind, k, -fdir).start()

    def one_c(k, kind):
        x_side(kind, k, 1 - c, fdir).wait_recv()
        part(kind, k, fdir).start()
        f_wait(kind, k).wait_recv()
        part(kind, k, 2).start()

    def stage_a(k, _):
        for kind in kinds:
            one_a(k, kind)
        return 0

    def stage_b(k, _):
        for kind in kinds:
            one_b(k, kind)
        return 0

    def to_other(kind, k):
        zz = at_z(-sgn * (k + 1)) if kind == 0 else at_z(sgn * (k + 1))
        return d2d(zz, 2 * k + kind)

    def stage_c(k, _):
        for kind in kinds:
            one_c(k, kind)
        return 0

    def backwards(stage, top):
        lax.fori_loop(0, hop, lambda i, _: stage(top - 1 - i, 0), 0)

    def far(stage):
        lax.fori_loop(0, last - hop, lambda i, _: stage(last - 1 - i, 0), 0)

    l_serve(0)
    l_serve(1)
    l_finish(0)
    l_serve(2)
    l_finish(1)
    l_ready(0)
    mix(0)
    for b in range(BUNDLES - 1, -1, -1):
        serve_relay(b)
    l_serve(3)
    l_finish(2)
    l_ready(1)
    mix(1)
    backwards(stage_a, hop)
    l_finish(3)
    l_ready(2)
    mix(2)
    backwards(stage_b, hop)
    l_ready(3)
    mix(3)
    backwards(stage_c, hop)
    antipode(functools.partial(one_a, last))
    far(stage_a)
    antipode(functools.partial(one_b, last))
    far(stage_b)
    antipode(functools.partial(one_c, last))
    far(stage_c)

    def other(zz, k):
        ref = units.at[pl.ds((zz * 2 + 1 - c) * per, per)]
        return rcopy(ref, ref, d_s.at[k], d_r.at[k], pside)

    other(z, n - 1).wait_recv()

    def stage_d(k, _):
        other(at_z(sgn * (k + 1)), 2 * k).wait_recv()
        other(at_z(-sgn * (k + 1)), 2 * k + 1).wait_recv()
        return 0

    lax.fori_loop(0, last, stage_d, 0)
    other(zhalf, 2 * last).wait_recv()

    lane = lax.broadcasted_iota(jnp.int32, (ROWS, LANES), 1)
    masks = [jnp.where(lane + h * LANES < kept_ref[0], 1.0, 0.0).astype(jnp.bfloat16) for h in range(thirds)]

    def place(j, _):
        i0, i1 = (jnp.clip(idx_ref[0, 2 * j + e], 0, units.shape[0] - thirds) for e in (0, 1))
        for h in range(thirds):
            two = jnp.concatenate([units[i0 + h], units[i1 + h]], axis=0)
            block[pl.ds(pl.multiple_of(j * ROWS, ROWS), ROWS), h * LANES : (h + 1) * LANES] = two * masks[h]
        return 0

    lax.fori_loop(0, block.shape[0] // ROWS, place, 0, unroll=4)

    nv = second.shape[0]
    cols = second.shape[2]
    turns = block.shape[0] // LANES // nv

    def mul(v, _):
        mine = block[:, pl.ds(pl.multiple_of(c * LANES, LANES), cols)]
        lhs = mixed[pl.ds(v * states, states)].reshape(states * width, states * width)
        second[v] = jnp.dot(lhs, mine, preferred_element_type=f32).astype(bf16)
        for k in range(turns):
            at = pl.multiple_of((v * turns + k) * LANES, LANES)
            flipped[:, pl.ds(at, LANES)] = block[pl.ds(at, LANES), :].T
        return 0

    lax.fori_loop(0, nv, mul, 0)
    share = out_ref.shape[1]

    def last_mul(v, _):
        res = jnp.dot(flipped[...], second[v], preferred_element_type=f32).T

        @pl.when(c == 0)
        def _():
            out_ref[v] = res[:share]

        @pl.when(c == 1)
        def _():
            out_ref[v] = res[cols - share :]

        return 0

    for v in range(nv):
        last_mul(v, 0)

    for b in range(BUNDLES):
        for cp in bundle(b):
            cp.wait_send()
    for g in range(parts):
        for cp in (*l_own(g), l_fwd(g), l_pair(0, g, c), l_pair(1, g, c), l_pair(2, g, c)):
            cp.wait_send()

    def drain(k, _):
        for cp in (
            rcopy(sent5.at[0], sent5.at[0], near5_s.at[k], near5_r.at[k], pside),
            rcopy(sent4.at[0], sent4.at[0], near4_s.at[k], near4_r.at[k], pside),
            *x_send(0, k), *x_send(1, k), f_send(0, k), f_send(1, k), to_other(0, k), to_other(1, k),
        ):
            cp.wait_send()
        return 0

    lax.fori_loop(0, last, drain, 0)

    def drain_last(kind):
        if kind == 0:
            rcopy(sent5.at[0], sent5.at[0], near5_s.at[last], near5_r.at[last], pside).wait_send()
        else:
            rcopy(sent4.at[0], sent4.at[0], near4_s.at[last], near4_r.at[last], pside).wait_send()
        for cp in (*x_send(kind, last), f_send(kind, last)):
            cp.wait_send()

    antipode(drain_last)
    d2d(zhalf, 2 * last).wait_send()
    d2d(z, n - 1).wait_send()


def on_device(held, owner_map, kept, left_env, mpo_tensor, mpo_mask, fields):
    n, nx, nc = lax.axis_size("env"), lax.axis_size("mpo"), lax.axis_size("col")
    pool, tile, width = held.shape
    sectors, tiles = owner_map.shape
    states = tiles * tile // width
    cap = 2 * tiles // (n * nc)
    thirds = width // LANES
    slab = left_env.shape[0]
    bond = mpo_tensor.shape[0]
    per = cap * thirds
    half, hop = n // 2, n // 4
    bf16 = jnp.bfloat16

    mpo_rows = jnp.transpose(mpo_tensor, (0, 2, 3, 1)).reshape(bond * states * states, bond)

    out = pl.pallas_call(
        functools.partial(main_kernel, (n, nx, cap, thirds, bond)),
        out_shape=jax.ShapeDtypeStruct((slab, width // nc, width), jnp.float32),
        in_specs=[
            pl.BlockSpec(memory_space=SMEM),
            pl.BlockSpec(memory_space=SMEM),
            pl.BlockSpec(memory_space=VMEM),
            pl.BlockSpec(memory_space=pl.ANY),
            pl.BlockSpec(memory_space=pl.ANY),
            pl.BlockSpec(memory_space=VMEM),
            pl.BlockSpec(memory_space=VMEM),
        ],
        out_specs=pl.BlockSpec(memory_space=VMEM),
        scratch_shapes=[
            VMEM((sectors, LANES), jnp.int32),
            VMEM((tile, 2 * LANES), jnp.int32),
            SMEM((sectors, LANES), jnp.int32),
            SMEM((tile, 2 * LANES), jnp.int32),
            VMEM((pool, tile, width), bf16),
            VMEM((n * nc * per, tile, LANES), bf16),
            VMEM((half, 5, tile, LANES), bf16),
            VMEM((half, 4, tile, LANES), bf16),
            VMEM((hop, 5, tile, LANES), bf16),
            VMEM((hop, 4, tile, LANES), bf16),
            VMEM((nx * slab, width, width), bf16),
            VMEM((slab * states * states * ROWS, 2 * bond * ROWS), bf16),
            VMEM((slab * states, width, states * width), bf16),
            VMEM((tiles * tile, width), bf16),
            VMEM((width, tiles * tile), bf16),
            VMEM((slab, states * width, 2 * LANES), bf16),
            DMA,
            DMA,
            DMA((2,)),
            DMA((half,)), DMA((half,)), DMA((half,)), DMA((half,)),
            DMA((2, BUNDLES)), DMA((2, BUNDLES)),
            DMA((2, 2, half)), DMA((2, 2, half)),
            DMA((2, half)), DMA((2, half)),
            DMA((n,)), DMA((n,)),
            DMA((2, 4)), DMA((2, 4)), DMA((4,)), DMA((4,)), DMA((3, 4)), DMA((3, 4)),
        ],
        compiler_params=pltpu.CompilerParams(collective_id=0, has_side_effects=True, vmem_limit_bytes=56 * 2**20),
        name="exchange_and_contract",
    )(kept, fields, owner_map, held, left_env[:, 0], mpo_rows, mpo_mask)
    return jnp.swapaxes(out, 1, 2)[:, None]


def solution(mesh):
    return jax.shard_map(
        on_device,
        mesh=mesh,
        in_specs=(
            P(("real", "env", "col"), None, None),
            P("real", None),
            P(("real", "env")),
            P("mpo", ("real", "env"), None, None),
            P(),
            P(),
            P("real"),
        ),
        out_specs=P("mpo", ("real", "env"), None, "col"),
        check_vma=False,
    )
```

```python
import functools

import jax
import jax.numpy as jnp
from jax import lax
from jax.experimental import pallas as pl
from jax.experimental.pallas import tpu as pltpu
from jax.sharding import PartitionSpec as P

MESH = pl.DeviceIdType.MESH
VMEM = pltpu.VMEM
SMEM = pltpu.SMEM
DMA = pltpu.SemaphoreType.DMA
LANES = 128
ROWS = 16
BUNDLES = 2


def find_tiles(pool, cap, thirds, map_ref, src_ref, idx_ref):
    tiles = map_ref.shape[1]
    row = lax.axis_index("env")
    me = row * lax.axis_size("col") + lax.axis_index("col")
    slots = map_ref[...]
    local = slots - me * pool
    mine = (local >= 0) & (local < pool)
    before = lax.broadcasted_iota(jnp.int32, (tiles, tiles), 0) < lax.broadcasted_iota(jnp.int32, (tiles, tiles), 1)
    rank = jnp.dot(
        jnp.where(mine, 1.0, 0.0).astype(jnp.bfloat16),
        jnp.where(before, 1.0, 0.0).astype(jnp.bfloat16),
        preferred_element_type=jnp.float32,
    )
    lane = lax.broadcasted_iota(jnp.int32, src_ref.shape, 1)
    found = jnp.zeros(src_ref.shape, jnp.float32)
    localf = local.astype(jnp.float32)
    for r in range(cap):
        slot = jnp.sum(jnp.where(mine & (rank == float(r)), localf, 0.0), axis=1, keepdims=True)
        found = jnp.where(lane == r, slot, found)
    src_ref[...] = jnp.clip(found.astype(jnp.int32), 0, pool - 1)
    own = map_ref[pl.ds(row, 1), :].astype(jnp.float32)
    owner = jnp.floor((own + 0.5) * (1.0 / pool))
    same = lax.broadcasted_iota(jnp.int32, (tiles, tiles), 0) == lax.broadcasted_iota(jnp.int32, (tiles, tiles), 1)
    column = jnp.sum(jnp.where(same, jnp.broadcast_to(owner, (tiles, tiles)), 0.0), axis=1, keepdims=True)
    order = jnp.sum(jnp.where((column == owner) & before, 1.0, 0.0), axis=0, keepdims=True)
    idx_ref[0:1, 0:tiles] = (owner * float(cap * thirds) + order * float(thirds)).astype(jnp.int32)


def main_kernel(
    dims, kept_ref, fields_ref, map_ref, pool_ref, left_ref, mpo_ref, mask_ref, out_ref,
    src_v, idx_v, src_ref, idx_ref, held_ref, units, sent5, sent4, relay5, relay4, lefts, kron, mixed, block, flipped, second,
    load_sem, pool_sem, table_sem, near5_s, near5_r, near4_s, near4_r, bund_s, bund_r, x_s, x_r, f_s, f_r, d_s, d_r,
    ln_s, ln_r, lf_s, lf_r, lp_s, lp_r,
):
    n, nx, cap, thirds, bond = dims
    per = cap * thirds
    slab = left_ref.shape[0]
    width = left_ref.shape[2]
    half = n // 2
    hop = n // 4
    z, x, c = lax.axis_index("env"), lax.axis_index("mpo"), lax.axis_index("col")
    states = block.shape[0] // width
    even = lax.rem(x + c, 2) == 0
    sgn = jnp.where(even, 1, -1)

    def start5(p):
        return 4 * p + p // 2

    def start4(p):
        return 5 * p - p // 2

    def at_z(off):
        return lax.rem(z + off + n, n)

    def at_x(off):
        return lax.rem(x + off + nx, nx)

    def rcopy(src, dst, ss, rs, where):
        return pltpu.make_async_remote_copy(src_ref=src, dst_ref=dst, send_sem=ss, recv_sem=rs, device_id=where, device_id_type=MESH)

    fetch = pltpu.make_async_copy(pool_ref, held_ref, pool_sem)
    fetch.start()
    load = pltpu.make_async_copy(left_ref, lefts.at[pl.ds(x * slab, slab)], load_sem)
    load.start()

    barrier = pltpu.get_barrier_semaphore()

    def greet(k, _):
        pl.semaphore_signal(barrier, inc=1, device_id={"env": at_z(k)}, device_id_type=MESH)
        pl.semaphore_signal(barrier, inc=1, device_id={"env": at_z(-k)}, device_id_type=MESH)
        return 0

    lax.fori_loop(1, hop + 1, greet, 0)
    pl.semaphore_signal(barrier, inc=1, device_id={"mpo": at_x(1)}, device_id_type=MESH)
    pl.semaphore_signal(barrier, inc=1, device_id={"mpo": at_x(-1)}, device_id_type=MESH)
    pl.semaphore_signal(barrier, inc=1, device_id={"col": 1 - c}, device_id_type=MESH)

    find_tiles(held_ref.shape[0], cap, thirds, map_ref, src_v, idx_v)
    tables = [
        pltpu.make_async_copy(src_v, src_ref, table_sem.at[0]),
        pltpu.make_async_copy(idx_v, idx_ref, table_sem.at[1]),
    ]
    for cp in tables:
        cp.start()

    def unit(t, u):
        r, h = u // thirds, lax.rem(u, thirds)
        at = jnp.clip(src_ref[t, r], 0, held_ref.shape[0] - 1)
        return held_ref[at, :, pl.ds(pl.multiple_of(h * LANES, LANES), LANES)]

    u5, u4 = start5(x), start4(x)

    def pick(k, _):
        t5, t4 = at_z(sgn * (k + 1)), at_z(-sgn * (k + 1))
        first = jnp.where(jnp.logical_and(k == half - 1, jnp.logical_not(even)), u4, u5)
        for i in range(5):
            sent5[k, i] = unit(t5, first + i)
        for i in range(4):
            sent4[k, i] = unit(t4, u4 + i)
        return 0

    for cp in tables:
        cp.wait()
    fetch.wait()
    lax.fori_loop(hop, half, pick, 0)
    load.wait()
    pl.semaphore_wait(barrier, 2 * hop + 3)

    def slot(zz, first, count):
        return units.at[pl.ds((zz * 2 + c) * per + first, count)]

    parts = ln_s.shape[1]
    piece = width // 2 // parts
    fdir = 1 - 2 * c
    pside = {"col": 1 - c}

    def rows_of(p, core, g):
        first = pl.multiple_of(core * (width // 2) + g * piece, ROWS)
        return lefts.at[pl.ds(p * slab, slab), pl.ds(first, piece)]

    def l_own(g):
        ref = rows_of(x, c, g)
        return [rcopy(ref, ref, ln_s.at[k, g], ln_r.at[k, g], {"mpo": at_x(off)}) for k, off in ((0, 1), (1, -1))]

    def l_fwd(g):
        ref = rows_of(at_x(-fdir), c, g)
        return rcopy(ref, ref, lf_s.at[g], lf_r.at[g], {"mpo": at_x(fdir)})

    def l_pair(k, g, core):
        ref = rows_of(at_x((-1, 1, 2)[k]), core, g)
        return rcopy(ref, ref, lp_s.at[k, g], lp_r.at[k, g], pside)

    def l_start(g):
        for cp in l_own(g):
            cp.start()

    def l_serve(g):
        for k, off in ((0, -1), (1, 1)):
            ref = rows_of(at_x(off), c, g)
            rcopy(ref, ref, ln_s.at[k, g], ln_r.at[k, g], pside).wait_recv()
        l_fwd(g).start()
        if g + 2 < parts:
            l_start(g + 2)
        l_pair(0, g, c).start()
        l_pair(1, g, c).start()

    def l_finish(g):
        ref = rows_of(at_x(2), c, g)
        rcopy(ref, ref, lf_s.at[g], lf_r.at[g], pside).wait_recv()
        l_pair(2, g, c).start()

    def l_ready(g):
        for k in range(3):
            l_pair(k, g, 1 - c).wait_recv()

    step = hop // BUNDLES

    def bundle(b):
        n4 = step - 1 if b == BUNDLES - 1 else step
        return (
            rcopy(sent5.at[pl.ds(hop + b * step, step)], relay5.at[pl.ds(b * step, step)], bund_s.at[0, b], bund_r.at[0, b], {"env": at_z(sgn * hop)}),
            rcopy(sent4.at[pl.ds(hop + b * step, n4)], relay4.at[pl.ds(b * step, n4)], bund_s.at[1, b], bund_r.at[1, b], {"env": at_z(-sgn * hop)}),
        )

    for b in range(BUNDLES - 1, -1, -1):
        for cp in bundle(b):
            cp.start()

    l_start(0)
    l_start(1)

    def near_copies(k):
        a = rcopy(sent5.at[k], slot(z, u5, 5), near5_s.at[k], near5_r.at[k], {"env": at_z(sgn * (k + 1))})
        b = rcopy(sent4.at[k], slot(z, u4, 4), near4_s.at[k], near4_r.at[k], {"env": at_z(-sgn * (k + 1))})
        return a, b

    def near(i, _):
        a, b = near_copies(hop - 1 - i)
        a.start()
        b.start()
        return 0

    lax.fori_loop(0, hop, pick, 0)
    lax.fori_loop(0, hop, near, 0)

    def own(u, _):
        units[(z * 2 + c) * per + u] = unit(z, u)
        return 0

    lax.fori_loop(0, per, own, 0)

    def d2d(zz, k):
        return rcopy(slot(zz, 0, per), slot(zz, 0, per), d_s.at[k], d_r.at[k], {"col": 1 - c})

    d2d(z, n - 1).start()

    rows, vees = mpo_ref.shape
    ss = states * states
    own_v = slab
    bf16, f32 = jnp.bfloat16, jnp.float32

    def iota(shape, dim):
        return lax.broadcasted_iota(jnp.int32, shape, dim)

    def ones(cond):
        return jnp.where(cond, 1.0, 0.0).astype(bf16)

    wrow = ones(iota((rows, bond), 0) // ss == iota((rows, bond), 1))
    base = mpo_ref[...] * jnp.dot(wrow, mask_ref[...].astype(f32).astype(bf16), preferred_element_type=f32)
    ri, li = iota((rows, vees), 0), iota((rows, vees), 1)
    qi, si = lax.rem(ri, ss) // states, lax.rem(ri, states)
    onsite = fields_ref[0] * (0.5 - (si // 2).astype(f32)) + fields_ref[1] * (0.5 - lax.rem(si, 2).astype(f32))
    base = base + jnp.where((ri >= (bond - 1) * ss) & (qi == si) & (li == 0), onsite, 0.0)
    high = base.astype(bf16)
    low = (base - high.astype(f32)).astype(bf16)
    nrow = ss * own_v
    select = ones(iota((nrow, vees), 1) == x * own_v + lax.rem(iota((nrow, vees), 0), own_v))
    match = lax.rem(iota((nrow, rows), 1), ss) == iota((nrow, rows), 0) // own_v
    spread = ones(iota((rows, bond * ROWS), 0) // ss == iota((rows, bond * ROWS), 1) // ROWS)

    def per_row(m):
        picked = lax.dot_general(select, m, (((1,), (1,)), ((), ())), preferred_element_type=f32)
        return jnp.dot(jnp.where(match, picked, 0.0).astype(bf16), spread, preferred_element_type=f32).astype(bf16)

    pairs = jnp.concatenate([per_row(high), per_row(low)], axis=1)
    kk = kron.shape[1]
    group = kron.shape[0] // 8
    diag = lax.rem(iota((group, kk), 0), ROWS) == lax.rem(iota((group, kk), 1), ROWS)

    def build(g, _):
        row = ones(iota((group, nrow), 0) // ROWS + g * (group // ROWS) == iota((group, nrow), 1))
        full = jnp.dot(row, pairs, preferred_element_type=f32)
        kron[pl.ds(g * group, group), :] = jnp.where(diag, full, 0.0).astype(bf16)
        return 0

    lax.fori_loop(0, 8, build, 0)

    chunk = kron.shape[0] // 2

    def mix(g):
        def one(t, _):
            r0 = pl.multiple_of(g * piece + t * ROWS, ROWS)
            r1 = pl.multiple_of(r0 + width // 2, ROWS)
            a = lefts[0:bond, pl.ds(r0, ROWS), :].reshape(bond * ROWS, width)
            b = lefts[0:bond, pl.ds(r1, ROWS), :].reshape(bond * ROWS, width)
            ab = jnp.concatenate([a, b], axis=1)
            ab = jnp.concatenate([ab, ab], axis=0)
            for e in range(2):
                res = jnp.dot(kron[e * chunk : (e + 1) * chunk, :], ab, preferred_element_type=f32).astype(bf16)
                for m in range(chunk // ROWS):
                    row = e * (chunk // ROWS) + m
                    qs, v = row // own_v, row % own_v
                    vq, s = v * states + qs // states, qs % states
                    part = res[m * ROWS : (m + 1) * ROWS, :]
                    mixed[vq, pl.ds(r0, ROWS), s * width : (s + 1) * width] = part[:, :width]
                    mixed[vq, pl.ds(r1, ROWS), s * width : (s + 1) * width] = part[:, width:]
            return 0

        lax.fori_loop(0, piece // ROWS, one, 0)

    def relay_copies(k):
        src5 = at_z(-sgn * hop)
        return rcopy(relay5.at[k], slot(src5, u5, 5), near5_s.at[hop + k], near5_r.at[hop + k], {"env": at_z(sgn * (k + 1))})

    def relay_last4():
        return rcopy(relay5.at[hop - 1, pl.ds(0, 4)], slot(at_z(-sgn * hop), u4, 4), near4_s.at[half - 1], near4_r.at[half - 1], {"env": at_z(sgn * hop)})

    def relay_copies4(k):
        src4 = at_z(sgn * hop)
        return rcopy(relay4.at[k], slot(src4, u4, 4), near4_s.at[hop + k], near4_r.at[hop + k], {"env": at_z(-sgn * (k + 1))})

    def serve_relay(b):
        for cp in bundle(b):
            cp.wait_recv()
        for k in range((b + 1) * step - 1, b * step - 1, -1):
            if k < hop - 1:
                relay_copies(k).start()
                relay_copies4(k).start()
            else:
                pl.when(even)(relay_copies(k).start)
                pl.when(jnp.logical_not(even))(relay_last4().start)

    def x_send(kind, k):
        zz = at_z(-sgn * (k + 1)) if kind == 0 else at_z(sgn * (k + 1))
        ref = slot(zz, u5, 5) if kind == 0 else slot(zz, u4, 4)
        return (
            rcopy(ref, ref, x_s.at[0, kind, k], x_r.at[0, 1 - kind, k], {"mpo": at_x(1)}),
            rcopy(ref, ref, x_s.at[1, kind, k], x_r.at[1, 1 - kind, k], {"mpo": at_x(-1)}),
        )

    def f_send(kind, k):
        zz = at_z(-sgn * (k + 1)) if kind == 0 else at_z(sgn * (k + 1))
        p = at_x(-fdir)
        ref = slot(zz, start4(p), 4) if kind == 0 else slot(zz, start5(p), 5)
        return rcopy(ref, ref, f_s.at[kind, k], f_r.at[1 - kind, k], {"mpo": at_x(fdir)})

    def f_wait(kind, k):
        zz = at_z(-sgn * (k + 1)) if kind == 0 else at_z(sgn * (k + 1))
        p = at_x(2)
        ref = slot(zz, start5(p), 5) if kind == 0 else slot(zz, start4(p), 4)
        return rcopy(ref, ref, f_s.at[kind, k], f_r.at[kind, k], {"mpo": at_x(1)})

    def z_wait(kind, k):
        zz = at_z(-sgn * (k + 1)) if kind == 0 else at_z(sgn * (k + 1))
        if kind == 0:
            return rcopy(sent5.at[0], slot(zz, u5, 5), near5_s.at[k], near5_r.at[k], {"env": at_z(1)})
        return rcopy(sent4.at[0], slot(zz, u4, 4), near4_s.at[k], near4_r.at[k], {"env": at_z(1)})

    zhalf = at_z(half)

    def antipode(stage):
        @pl.when(even)
        def _():
            stage(0)

        @pl.when(jnp.logical_not(even))
        def _():
            stage(1)

    kinds = (0, 1)
    last = half - 1

    def part(kind, k, off):
        zz = at_z(-sgn * (k + 1)) if kind == 0 else at_z(sgn * (k + 1))
        p = at_x(off)
        five = (kind == 0) == (isinstance(off, int) and off % 2 == 0)
        ref = slot(zz, start5(p), 5) if five else slot(zz, start4(p), 4)
        at = 2 * last if isinstance(k, int) and k == last else 2 * k + kind
        return rcopy(ref, ref, d_s.at[at], d_r.at[at], pside)

    def one_a(k, kind):
        z_wait(kind, k).wait_recv()
        for cp in x_send(kind, k):
            cp.start()
        part(kind, k, 0).start()

    def x_side(kind, k, side, off):
        zz = at_z(-sgn * (k + 1)) if kind == 0 else at_z(sgn * (k + 1))
        ref = slot(zz, start4(at_x(off)), 4) if kind == 0 else slot(zz, start5(at_x(off)), 5)
        return rcopy(ref, ref, x_s.at[side, kind, k], x_r.at[side, kind, k], pside)

    def one_b(k, kind):
        x_side(kind, k, c, -fdir).wait_recv()
        f_send(kind, k).start()
        part(kind, k, -fdir).start()

    def one_c(k, kind):
        x_side(kind, k, 1 - c, fdir).wait_recv()
        part(kind, k, fdir).start()
        f_wait(kind, k).wait_recv()
        part(kind, k, 2).start()

    def stage_a(k, _):
        for kind in kinds:
            one_a(k, kind)
        return 0

    def stage_b(k, _):
        for kind in kinds:
            one_b(k, kind)
        return 0

    def to_other(kind, k):
        zz = at_z(-sgn * (k + 1)) if kind == 0 else at_z(sgn * (k + 1))
        return d2d(zz, 2 * k + kind)

    def stage_c(k, _):
        for kind in kinds:
            one_c(k, kind)
        return 0

    def backwards(stage, top):
        lax.fori_loop(0, hop, lambda i, _: stage(top - 1 - i, 0), 0)

    def far(stage):
        lax.fori_loop(0, last - hop, lambda i, _: stage(last - 1 - i, 0), 0)

    l_serve(0)
    l_serve(1)
    l_finish(0)
    l_serve(2)
    l_finish(1)
    l_ready(0)
    mix(0)
    l_serve(3)
    l_finish(2)
    l_ready(1)
    mix(1)
    for b in range(BUNDLES - 1, -1, -1):
        serve_relay(b)
    backwards(stage_a, hop)
    l_finish(3)
    l_ready(2)
    mix(2)
    backwards(stage_b, hop)
    l_ready(3)
    mix(3)
    backwards(stage_c, hop)
    antipode(functools.partial(one_a, last))
    far(stage_a)
    antipode(functools.partial(one_b, last))
    far(stage_b)
    antipode(functools.partial(one_c, last))
    far(stage_c)

    def other(zz, k):
        ref = units.at[pl.ds((zz * 2 + 1 - c) * per, per)]
        return rcopy(ref, ref, d_s.at[k], d_r.at[k], pside)

    other(z, n - 1).wait_recv()

    def stage_d(k, _):
        other(at_z(sgn * (k + 1)), 2 * k).wait_recv()
        other(at_z(-sgn * (k + 1)), 2 * k + 1).wait_recv()
        return 0

    lax.fori_loop(0, last, stage_d, 0)
    other(zhalf, 2 * last).wait_recv()

    lane = lax.broadcasted_iota(jnp.int32, (ROWS, LANES), 1)
    masks = [jnp.where(lane + h * LANES < kept_ref[0], 1.0, 0.0).astype(jnp.bfloat16) for h in range(thirds)]

    def place(j, _):
        i0, i1 = (jnp.clip(idx_ref[0, 2 * j + e], 0, units.shape[0] - thirds) for e in (0, 1))
        for h in range(thirds):
            two = jnp.concatenate([units[i0 + h], units[i1 + h]], axis=0)
            block[pl.ds(pl.multiple_of(j * ROWS, ROWS), ROWS), h * LANES : (h + 1) * LANES] = two * masks[h]
        return 0

    lax.fori_loop(0, block.shape[0] // ROWS, place, 0, unroll=4)

    nv = second.shape[0]
    cols = second.shape[2]
    turns = block.shape[0] // LANES // nv

    def mul(v, _):
        mine = block[:, pl.ds(pl.multiple_of(c * LANES, LANES), cols)]
        lhs = mixed[pl.ds(v * states, states)].reshape(states * width, states * width)
        second[v] = jnp.dot(lhs, mine, preferred_element_type=f32).astype(bf16)
        for k in range(turns):
            at = pl.multiple_of((v * turns + k) * LANES, LANES)
            flipped[:, pl.ds(at, LANES)] = block[pl.ds(at, LANES), :].T
        return 0

    lax.fori_loop(0, nv, mul, 0)
    share = out_ref.shape[1]

    def last_mul(v, _):
        res = jnp.dot(flipped[...], second[v], preferred_element_type=f32).T

        @pl.when(c == 0)
        def _():
            out_ref[v] = res[:share]

        @pl.when(c == 1)
        def _():
            out_ref[v] = res[cols - share :]

        return 0

    for v in range(nv):
        last_mul(v, 0)

    for b in range(BUNDLES):
        for cp in bundle(b):
            cp.wait_send()
    for g in range(parts):
        for cp in (*l_own(g), l_fwd(g), l_pair(0, g, c), l_pair(1, g, c), l_pair(2, g, c)):
            cp.wait_send()

    def drain(k, _):
        for cp in (
            rcopy(sent5.at[0], sent5.at[0], near5_s.at[k], near5_r.at[k], pside),
            rcopy(sent4.at[0], sent4.at[0], near4_s.at[k], near4_r.at[k], pside),
            *x_send(0, k), *x_send(1, k), f_send(0, k), f_send(1, k), to_other(0, k), to_other(1, k),
        ):
            cp.wait_send()
        return 0

    lax.fori_loop(0, last, drain, 0)

    def drain_last(kind):
        if kind == 0:
            rcopy(sent5.at[0], sent5.at[0], near5_s.at[last], near5_r.at[last], pside).wait_send()
        else:
            rcopy(sent4.at[0], sent4.at[0], near4_s.at[last], near4_r.at[last], pside).wait_send()
        for cp in (*x_send(kind, last), f_send(kind, last)):
            cp.wait_send()

    antipode(drain_last)
    d2d(zhalf, 2 * last).wait_send()
    d2d(z, n - 1).wait_send()


def on_device(held, owner_map, kept, left_env, mpo_tensor, mpo_mask, fields):
    n, nx, nc = lax.axis_size("env"), lax.axis_size("mpo"), lax.axis_size("col")
    pool, tile, width = held.shape
    sectors, tiles = owner_map.shape
    states = tiles * tile // width
    cap = 2 * tiles // (n * nc)
    thirds = width // LANES
    slab = left_env.shape[0]
    bond = mpo_tensor.shape[0]
    per = cap * thirds
    half, hop = n // 2, n // 4
    bf16 = jnp.bfloat16

    mpo_rows = jnp.transpose(mpo_tensor, (0, 2, 3, 1)).reshape(bond * states * states, bond)

    out = pl.pallas_call(
        functools.partial(main_kernel, (n, nx, cap, thirds, bond)),
        out_shape=jax.ShapeDtypeStruct((slab, width // nc, width), jnp.float32),
        in_specs=[
            pl.BlockSpec(memory_space=SMEM),
            pl.BlockSpec(memory_space=SMEM),
            pl.BlockSpec(memory_space=VMEM),
            pl.BlockSpec(memory_space=pl.ANY),
            pl.BlockSpec(memory_space=pl.ANY),
            pl.BlockSpec(memory_space=VMEM),
            pl.BlockSpec(memory_space=VMEM),
        ],
        out_specs=pl.BlockSpec(memory_space=VMEM),
        scratch_shapes=[
            VMEM((sectors, LANES), jnp.int32),
            VMEM((tile, 2 * LANES), jnp.int32),
            SMEM((sectors, LANES), jnp.int32),
            SMEM((tile, 2 * LANES), jnp.int32),
            VMEM((pool, tile, width), bf16),
            VMEM((n * nc * per, tile, LANES), bf16),
            VMEM((half, 5, tile, LANES), bf16),
            VMEM((half, 4, tile, LANES), bf16),
            VMEM((hop, 5, tile, LANES), bf16),
            VMEM((hop, 4, tile, LANES), bf16),
            VMEM((nx * slab, width, width), bf16),
            VMEM((slab * states * states * ROWS, 2 * bond * ROWS), bf16),
            VMEM((slab * states, width, states * width), bf16),
            VMEM((tiles * tile, width), bf16),
            VMEM((width, tiles * tile), bf16),
            VMEM((slab, states * width, 2 * LANES), bf16),
            DMA,
            DMA,
            DMA((2,)),
            DMA((half,)), DMA((half,)), DMA((half,)), DMA((half,)),
            DMA((2, BUNDLES)), DMA((2, BUNDLES)),
            DMA((2, 2, half)), DMA((2, 2, half)),
            DMA((2, half)), DMA((2, half)),
            DMA((n,)), DMA((n,)),
            DMA((2, 4)), DMA((2, 4)), DMA((4,)), DMA((4,)), DMA((3, 4)), DMA((3, 4)),
        ],
        compiler_params=pltpu.CompilerParams(collective_id=0, has_side_effects=True, vmem_limit_bytes=56 * 2**20),
        name="exchange_and_contract",
    )(kept, fields, owner_map, held, left_env[:, 0], mpo_rows, mpo_mask)
    return jnp.swapaxes(out, 1, 2)[:, None]


def solution(mesh):
    return jax.shard_map(
        on_device,
        mesh=mesh,
        in_specs=(
            P(("real", "env", "col"), None, None),
            P("real", None),
            P(("real", "env")),
            P("mpo", ("real", "env"), None, None),
            P(),
            P(),
            P("real"),
        ),
        out_specs=P("mpo", ("real", "env"), None, "col"),
        check_vma=False,
    )
```
